32 devices in a mesh: seq: 8 (over z, core), vocab: 4 (over y, x).
Axes of the slice: x: 2, y: 2, z: 4, core: 2. Of those that a mesh axis runs over, the one named last changes fastest.
Arguments:
- probe_states: bfloat16 [3, 8192, 6144], P(None, 'seq', 'vocab'), may hold values from -6 to 6
- final_states: bfloat16 [8192, 6144], P('seq', 'vocab'), may hold values from -6 to 6
- translator: bfloat16 [3, 6144, 6144], P(None, 'vocab', 'seq'), may hold values from -0.078125 to 0.078125
- translator_bias: float32 [3, 6144], P(None, 'seq'), may hold values from -4 to 4
- norm_gain: float32 [6144], P('seq'), may hold values from 0.5 to 1.5
- unembed: bfloat16 [32768, 6144], P('vocab', 'seq'), may hold values from -0.21875 to 0.21875
- answer_rows: int32 [8, 32], P('seq'), may hold values from 0 to 1023, as said below
- answer_count: int32 [8], P('seq'), may hold values from 1 to 32, 128 in all
- targets: int32 [8, 32], P('seq'), may hold values from 0 to 32767
Outputs:
- answer_logprob: float32 [4, 8, 32], P(None, 'seq')
- answer_kl: float32 [3, 8, 32], P(None, 'seq')
The draws below stay inside these ranges and needn't reach their ends.
Inputs may be any that keep to these rules, and one draw needn't show every extreme that they name: `answer_rows`: each row holds 32 different positions. `answer_count`: the counts sum to 128, and some sequence has 32.
All inputs are finite; a program needn't handle non-finite values. No bound on the sum of `answer_count` on one device may be relied on, other than what follows from the above.
Results may differ from the reference program's by a relative error of at most 0.00099.
Values may be sent and summed in bfloat16 or wider, within the bound.
A program may use at most 128 MiB of HBM per device.

```python
import math
import jax
import jax.numpy as jnp
import numpy as np
from jax import lax

D = 6144
V = 32768
LAYERS = 3
LENGTH = 1024
CAP = 32
SEQS = 8
TOKENS = 8192
FLAGGED = 128


def draw_answer_rows(key, part):
    seqs = TOKENS // LENGTH
    scores = jax.random.randint(key, (seqs, LENGTH), 0, 1 << 20)
    scores = scores * LENGTH + jnp.arange(LENGTH, dtype=jnp.int32)[None, :]
    order = jnp.argsort(scores, axis=1)
    return order[:, :CAP].astype(jnp.int32)


def place_ends(drawn, stream_key, least, high):
    spot = [jax.random.randint(jax.random.fold_in(stream_key, axis), (), 0, length) for axis, length in enumerate(drawn.shape)]
    widest = drawn.shape.index(max(drawn.shape))
    neighbour = spot[:widest] + [(spot[widest] + 1) % drawn.shape[widest]] + spot[widest + 1:]
    return drawn.at[tuple(spot)].set(least).at[tuple(neighbour)].set(high)


def block_scale(key, extent, shards, least, largest):
    def one(dim, blocks):
        heights = jax.random.uniform(jax.random.fold_in(jax.random.fold_in(key, 6), dim), (blocks,), jnp.float32, least / len(shards), largest / len(shards))
        return jnp.repeat(jnp.exp(heights), extent[dim] // blocks).reshape((-1,) + (1,) * (len(extent) - dim - 1))

    gain = one(*shards[0])
    for cut in shards[1:]:
        gain = gain * one(*cut)
    return gain


def rank_table(number_of, lean):
    weights = [(1 << 20) // math.isqrt(standing ** lean) + 1 for standing in range(1, number_of + 1)]
    scale = 1 + sum(weights) // (1 << 30)
    return np.cumsum(np.array([max(1, weight // scale) for weight in weights]))


def ranked(stream_key, extent, number_of, lean):
    grid = rank_table(number_of, lean)
    ticket = jax.random.randint(jax.random.fold_in(stream_key, 1), extent, 0, int(grid[number_of - 1]))
    rank = jnp.searchsorted(jnp.asarray(grid, jnp.int32), ticket, side="right")
    return jax.random.permutation(jax.random.fold_in(stream_key, 2), number_of)[rank].astype(jnp.int32)


def length_profile(count, total, bound, skew):
    weights = [(1 << 20) // math.isqrt(rank ** skew) + 1 for rank in range(2, count + 1)]
    rest, counts = total - bound - (count - 1), [1] * (count - 1)
    while rest > 0:
        free = [i for i in range(count - 1) if counts[i] < bound]
        mass, budget = sum([weights[i] for i in free]), rest
        for i in free:
            extra = min(bound - counts[i], max(1, budget * weights[i] // mass), rest)
            counts[i] = counts[i] + extra
            rest = rest - extra
    return np.array([bound] + counts)


def ragged_sizes(key, amount, total, most, lean):
    if amount == 2:
        one = jax.random.randint(key, (), max(1, total - most), min(most, total - 1) + 1)
        return jnp.stack([one, total - one])
    tallies = jnp.asarray(length_profile(amount, total, most, lean), jnp.int32)
    twos = (amount - 1) // 2
    giver, receiver = tallies[1:1 + 2 * twos:2], tallies[2:2 + 2 * twos:2]
    room = jnp.minimum(giver - 1, most - receiver)
    shifted = jax.random.randint(jax.random.fold_in(key, 1), (twos,), 0, 1 << 20) % (room + 1)
    tallies = tallies.at[1:1 + 2 * twos:2].set(giver - shifted).at[2:2 + 2 * twos:2].set(receiver + shifted)
    return tallies[jax.random.permutation(jax.random.fold_in(key, 2), amount)]


def gaussian(own_key, dims, deviation, reach, split=(), kind=jnp.bfloat16):
    result = deviation * jax.random.normal(own_key, dims, jnp.float32)
    if split:
        result = result * block_scale(own_key, dims, split, -0.22, 0.18)
    return jnp.clip(result, -reach, reach).astype(kind)


def setup_inputs(seed: int = 0) -> dict:
    key_of = jax.random.split(jax.random.key(seed), 10)
    probe_states = gaussian(key_of[0], (LAYERS, TOKENS, D), 1.0, 6.0, ((1, 8), (2, 4)))
    final_states = gaussian(key_of[1], (TOKENS, D), 1.0, 6.0, ((0, 8), (1, 4)))
    translator = gaussian(key_of[2], (LAYERS, D, D), D ** -0.5, 0.078125, ((1, 4), (2, 8)))
    translator_bias = gaussian(key_of[3], (LAYERS, D), 0.5, 4.0, ((1, 8),), jnp.float32)
    norm_gain = jnp.clip(1.0 + 0.1 * jax.random.normal(key_of[4], (D,), jnp.float32), 0.5, 1.5)
    unembed = gaussian(key_of[5], (V, D), (D // 9) ** -0.5, 0.21875, ((0, 4), (1, 8)))
    answer_rows = draw_answer_rows(jax.random.fold_in(key_of[9], 71), 0)
    answer_count = ragged_sizes(key_of[7], SEQS, FLAGGED, CAP, 2).astype(jnp.int32)
    targets = place_ends(ranked(key_of[8], (SEQS, CAP), V, 2), jax.random.fold_in(key_of[8], 3), 0, V - 1).astype(jnp.int32)
    return {"probe_states": probe_states, "final_states": final_states, "translator": translator, "translator_bias": translator_bias, "norm_gain": norm_gain, "unembed": unembed, "answer_rows": answer_rows, "answer_count": answer_count, "targets": targets}


def lens_logits(rows, norm_gain, unembed_f):
    mean_sq = lax.optimization_barrier(jnp.mean(rows * rows, axis=-1))
    scaled = (rows * norm_gain).astype(jnp.bfloat16)
    raw = jnp.dot(scaled.astype(jnp.float32), unembed_f.T, precision=lax.Precision.HIGHEST)
    return raw * lax.rsqrt(mean_sq + 1e-05)[:, None]

def reference(probe_states, final_states, translator, translator_bias, norm_gain, unembed, answer_rows, answer_count, targets):
    seqs = answer_rows.shape[0]
    flat = (jnp.arange(seqs, dtype=jnp.int32)[:, None] * LENGTH + answer_rows.astype(jnp.int32)).reshape(-1)
    live = (jnp.arange(CAP, dtype=jnp.int32)[None, :] < answer_count[:, None]).reshape(-1)
    wanted = targets.reshape(-1)[:, None]
    unembed_f = unembed.astype(jnp.float32)
    final_rows = jnp.take(final_states, flat, axis=0).astype(jnp.float32)
    final_logits = lens_logits(final_rows, norm_gain, unembed_f)
    final_lse = jnp.log(lax.optimization_barrier(jnp.sum(jnp.exp(final_logits), axis=-1)))
    final_prob = jnp.exp(final_logits - final_lse[:, None])
    logprobs = []
    divergences = []
    for layer in range(LAYERS):
        rows = jnp.take(probe_states[layer], flat, axis=0)
        lensed = rows.astype(jnp.float32) + jnp.dot(rows.astype(jnp.float32), translator[layer].astype(jnp.float32), precision=lax.Precision.HIGHEST) + translator_bias[layer]
        logits = lens_logits(lensed, norm_gain, unembed_f)
        lse = jnp.log(lax.optimization_barrier(jnp.sum(jnp.exp(logits), axis=-1)))
        logprobs.append(jnp.take_along_axis(logits, wanted, axis=1)[:, 0] - lse)
        divergences.append(lax.optimization_barrier(jnp.sum(final_prob * (final_logits - logits), axis=-1)) - final_lse + lse)
    logprobs.append(jnp.take_along_axis(final_logits, wanted, axis=1)[:, 0] - final_lse)
    logprob = jnp.where(live[None, :], jnp.stack(logprobs), 0.0).reshape(LAYERS + 1, seqs, CAP)
    divergence = jnp.where(live[None, :], jnp.stack(divergences), 0.0).reshape(LAYERS, seqs, CAP)
    return (logprob, divergence)
```

```python
import math
import jax
import jax.numpy as jnp
from jax import lax
from jax.experimental import pallas as pl
from jax.experimental.pallas import tpu as pltpu
from jax.sharding import PartitionSpec as P

FLAG_DEV = 16
STATE_MAX, MATRIX_MAX, BIAS_MAX, GAIN_MAX, UNEMBED_MAX = 6.0, 0.078125, 4.0, 1.5, 0.21875
CHUNKS = 4
LAG = 2
SLOTS = 4
MESH = pl.DeviceIdType.MESH
f32, bf16, i16, i32 = jnp.float32, jnp.bfloat16, jnp.int16, jnp.int32


class Code:
    def __init__(self, model):
        widest = GAIN_MAX * UNEMBED_MAX * model * (STATE_MAX + BIAS_MAX + model * STATE_MAX * MATRIX_MAX)
        self.knee = 7.5e-4
        self.scale = 32700.0 / math.log2(1.0 + 1.02 * widest / self.knee)

    def enc(self, value):
        level = jnp.log2(1.0 + jnp.abs(value) * (1.0 / self.knee)) * self.scale
        return jnp.round(jnp.where(value < 0, -level, level)).astype(i32).astype(i16)

    def dec(self, code):
        level = code.astype(i32).astype(f32)
        size = (jnp.exp2(jnp.abs(level) * (1.0 / self.scale)) - 1.0) * self.knee
        return jnp.where(level < 0, -size, size)


def kernel(
    layers, total, seq_count, vocab_count, code,
    y_ref, fac_ref, tgt_ref, u_hbm, out_ref,
    u, own, psend, precv, zsend, zrecv, z3, e3, acc, stat_send, stat_recv, line_send, line_recv,
    u_sem, psend_sem, precv_sem, zsend_sem, zrecv_sem, ssend_sem, srecv_sem, lsend_sem, lrecv_sem,
):
    seq, voc = lax.axis_index("seq"), lax.axis_index("vocab")
    chip, core = seq // 2, seq % 2
    chips = seq_count // 2
    vp, _ = u.shape
    half, quarter = vp // 2, vp // 4
    chunk = quarter // CHUNKS
    steps = layers * CHUNKS
    plane = 2 * vocab_count
    me = core * vocab_count + voc
    at_end = jnp.logical_or(chip == 0, chip == chips - 1)

    pieces = 4 * CHUNKS
    piece = vp // pieces

    def u_copy(k):
        rows = pl.ds(pl.multiple_of(k * piece, piece), piece)
        return pltpu.make_async_copy(u_hbm.at[rows], u.at[rows], u_sem.at[k])

    @pl.loop(0, pieces)
    def _(k):
        u_copy(k).start()

    barrier = pltpu.get_barrier_semaphore()

    def in_plane(p):
        q = lax.rem(me + p, plane)
        return q, (chip * 2 + q // vocab_count, lax.rem(q, vocab_count))

    def in_line(p):
        q = lax.rem(chip + p, chips)
        return q, (q * 2 + core, voc)

    @pl.loop(1, plane)
    def _(p):
        pl.semaphore_signal(barrier, inc=1, device_id=in_plane(p)[1], device_id_type=MESH)

    @pl.loop(1, chips)
    def _(p):
        pl.semaphore_signal(barrier, inc=1, device_id=in_line(p)[1], device_id_type=MESH)

    pl.semaphore_wait(barrier, plane - 1 + chips - 1)
    acc[...] = jnp.zeros_like(acc)

    def pair_copy(t):
        return pltpu.make_async_remote_copy(
            src_ref=psend.at[lax.rem(t, SLOTS)], dst_ref=precv.at[t],
            send_sem=psend_sem.at[lax.rem(t, SLOTS)], recv_sem=precv_sem.at[t],
            device_id=(chip * 2 + 1 - core, voc), device_id_type=MESH,
        )

    def line_copy(k, d):
        to = jnp.minimum(chip + 1, chips - 1) if d == 0 else jnp.maximum(chip - 1, 0)
        return pltpu.make_async_remote_copy(
            src_ref=zsend.at[k, d], dst_ref=zrecv.at[k, d],
            send_sem=zsend_sem.at[k, d], recv_sem=zrecv_sem.at[k, d],
            device_id=(to * 2 + core, voc), device_id_type=MESH,
        )

    def rows_at(owner, d, j):
        start = owner * half + d * quarter + j * chunk
        return pl.ds(pl.multiple_of(start, chunk), chunk)

    def product(rows, yl):
        return lax.dot_general(u[rows, :], yl, (((1,), (1,)), ((), ())), preferred_element_type=f32)

    def fold(value):
        return jnp.sum(value.reshape(chunk // 8, 8, total), axis=0)

    def finish(k, d, value):
        rank, j = k // CHUNKS, lax.rem(k, CHUNKS)
        layer = lax.rem(rank + layers - 1, layers)
        logit = value * fac_ref[layer]
        base = voc * vp + core * half + d * quarter + j * chunk
        spot = lax.broadcasted_iota(i32, (chunk, total), 0) + base
        grown = jnp.exp(logit)
        acc[layer] += fold(grown)
        acc[layers + layer] += fold(jnp.where(spot == tgt_ref[...], logit, 0.0))

        @pl.when(rank == 0)
        def _():
            z3[j] = logit
            e3[j] = grown

        @pl.when(rank > 0)
        def _():
            acc[2 * layers + layer] += fold(e3[j] * (z3[j] - logit))

    def forward(k, d):
        first = chip == (0 if d == 0 else chips - 1)
        last = chip == (chips - 1 if d == 0 else 0)

        @pl.when(jnp.logical_not(first))
        def _():
            line_copy(k, d).wait_recv()
            own[k, d] = own[k, d] + code.dec(zrecv[k, d])

        @pl.when(jnp.logical_not(last))
        def _():
            zsend[k, d] = code.enc(own[k, d])
            line_copy(k, d).start()

        @pl.when(last)
        def _():
            finish(k, d, own[k, d])

    @pl.loop(0, steps + 1 + LAG * (chips - 1))
    def _(t):
        @pl.when(t < CHUNKS)
        def _():
            for part in range(4):
                u_copy(part * CHUNKS + t).wait()

        @pl.when(t < steps)
        def _():
            layer, j = lax.rem(t // CHUNKS + layers - 1, layers), lax.rem(t, CHUNKS)
            yl = y_ref[pl.ds(pl.multiple_of(layer * total, total), total), :]

            @pl.when(t >= SLOTS)
            def _():
                pair_copy(t - SLOTS).wait_send()

            for d in range(2):
                psend[lax.rem(t, SLOTS), d] = product(rows_at(1 - core, d, j), yl)
            pair_copy(t).start()
            for d in range(2):
                own[t, d] = product(rows_at(core, d, j), yl)

        @pl.when(jnp.logical_and(t >= 1, t <= steps))
        def _():
            pair_copy(t - 1).wait_recv()
            own[t - 1] = own[t - 1] + precv[t - 1]

        for d in range(2):
            k = t - 1 - LAG * (chip if d == 0 else chips - 1 - chip)

            @pl.when(jnp.logical_and(k >= 0, k < steps))
            def _():
                forward(k, d)

    @pl.loop(steps - SLOTS, steps)
    def _(t):
        pair_copy(t).wait_send()

    @pl.loop(0, steps)
    def _(k):
        for d in range(2):
            @pl.when(chip != (chips - 1 if d == 0 else 0))
            def _():
                line_copy(k, d).wait_send()

    def stat_copy(p):
        _, there = in_plane(p)
        return pltpu.make_async_remote_copy(
            src_ref=stat_send, dst_ref=stat_recv.at[me], send_sem=ssend_sem.at[p], recv_sem=srecv_sem.at[me],
            device_id=there, device_id_type=MESH,
        )

    def stat_arrival(p):
        q, there = in_plane(p)
        return pltpu.make_async_remote_copy(
            src_ref=stat_send, dst_ref=stat_recv.at[q], send_sem=ssend_sem.at[p], recv_sem=srecv_sem.at[q],
            device_id=there, device_id_type=MESH,
        )

    end = jnp.where(chip == 0, 0, 1)

    def line_stat(p):
        _, there = in_line(p)
        return pltpu.make_async_remote_copy(
            src_ref=line_send, dst_ref=line_recv.at[end], send_sem=lsend_sem.at[p], recv_sem=lrecv_sem.at[end],
            device_id=there, device_id_type=MESH,
        )

    def line_arrival(side):
        return pltpu.make_async_remote_copy(
            src_ref=line_send, dst_ref=line_recv.at[side], send_sem=lsend_sem.at[0], recv_sem=lrecv_sem.at[side],
            device_id=in_line(1)[1], device_id_type=MESH,
        )

    @pl.when(at_end)
    def _():
        stat = jnp.concatenate(
            [jnp.sum(acc[i], axis=0, keepdims=True) for i in range(3 * layers)]
            + [jnp.zeros((stat_send.shape[0] - 3 * layers, total), f32)], axis=0,
        )
        stat_send[...] = stat
        stat_recv[me] = stat

        @pl.loop(1, plane)
        def _(p):
            stat_copy(p).start()

        @pl.loop(1, plane)
        def _(p):
            stat_arrival(p).wait_recv()

        full = stat_recv[0]
        for q in range(1, plane):
            full = full + stat_recv[q]
        line_send[...] = full
        line_recv[end] = full

        @pl.loop(1, chips)
        def _(p):
            line_stat(p).start()

        @pl.loop(1, plane)
        def _(p):
            stat_copy(p).wait_send()

    for side in range(2):
        @pl.when(chip != (0 if side == 0 else chips - 1))
        def _():
            line_arrival(side).wait_recv()

    @pl.when(at_end)
    def _():
        @pl.loop(1, chips)
        def _(p):
            line_stat(p).wait_send()

    full = line_recv[0] + line_recv[1]
    total_exp, picked = full[:layers], full[layers : 2 * layers]
    cross = full[2 * layers : 3 * layers - 1]
    log_total = jnp.log(total_exp)
    gone = cross / total_exp[layers - 1 :] - log_total[layers - 1 :] + log_total[: layers - 1]
    spare = jnp.zeros((out_ref.shape[0] - 2 * layers + 1, total), f32)
    out_ref[...] = jnp.concatenate([picked - log_total, gone, spare], axis=0)


def readout(y, fac, tgt, unembed, layers, total, seq_count, vocab_count, model):
    vp, width = unembed.shape
    steps = layers * CHUNKS
    chunk = vp // 4 // CHUNKS
    plane = 2 * vocab_count
    code = Code(model)
    deep = -(-3 * layers // 8) * 8
    dma = pltpu.SemaphoreType.DMA
    vmem = pl.BlockSpec(memory_space=pltpu.VMEM)
    body = lambda *refs: kernel(layers, total, seq_count, vocab_count, code, *refs)
    return pl.pallas_call(
        body,
        out_shape=jax.ShapeDtypeStruct((deep, total), f32),
        in_specs=[vmem, vmem, vmem, pl.BlockSpec(memory_space=pl.ANY)],
        out_specs=vmem,
        scratch_shapes=[
            pltpu.VMEM((vp, width), bf16),
            pltpu.VMEM((steps, 2, chunk, total), f32),
            pltpu.VMEM((SLOTS, 2, chunk, total), f32),
            pltpu.VMEM((steps, 2, chunk, total), f32),
            pltpu.VMEM((steps, 2, chunk, total), i16),
            pltpu.VMEM((steps, 2, chunk, total), i16),
            pltpu.VMEM((CHUNKS, chunk, total), f32),
            pltpu.VMEM((CHUNKS, chunk, total), f32),
            pltpu.VMEM((3 * layers, 8, total), f32),
            pltpu.VMEM((deep, total), f32),
            pltpu.VMEM((plane, deep, total), f32),
            pltpu.VMEM((deep, total), f32),
            pltpu.VMEM((2, deep, total), f32),
            dma((4 * CHUNKS,)),
            dma((SLOTS,)),
            dma((steps,)),
            dma((steps, 2)),
            dma((steps, 2)),
            dma((plane,)),
            dma((plane,)),
            dma((seq_count // 2,)),
            dma((2,)),
        ],
        compiler_params=pltpu.CompilerParams(
            collective_id=0, has_side_effects=True, vmem_limit_bytes=62 << 20
        ),
        name="readout",
    )(y, fac, tgt, unembed)


def body(
    probe_states,
    final_states,
    translator,
    translator_bias,
    norm_gain,
    unembed,
    answer_rows,
    answer_count,
    targets,
):
    f32 = jnp.float32
    bf16 = jnp.bfloat16
    seq_count = lax.axis_size("seq")
    vocab_count = lax.axis_size("vocab")
    seq_index = lax.axis_index("seq")
    vocab_index = lax.axis_index("vocab")
    layers = probe_states.shape[0]
    cap = answer_rows.shape[1]
    width_in = probe_states.shape[2]
    width_out = translator.shape[2]
    vocab_part = unembed.shape[0]
    model = width_in * vocab_count
    total = seq_count * FLAG_DEV
    stacked = (layers + 1) * total
    picks = answer_rows[0]

    probed = jnp.take(probe_states, picks, axis=1, mode="clip")
    local = jnp.concatenate(
        [probed[l] for l in range(layers)] + [jnp.take(final_states, picks, axis=0, mode="clip")],
        axis=1,
    )
    gathered = lax.all_gather(local, "seq", axis=0, tiled=True)
    meta = lax.all_gather(
        jnp.concatenate([answer_count[None, :], targets], axis=1), "seq", axis=0, tiled=True
    )
    counts, targets_all = meta[:, 0], meta[:, 1:]
    order = jnp.arange(seq_count, dtype=jnp.int32)
    starts = jnp.sum(jnp.where(order[:, None] < order[None, :], counts[:, None], 0), axis=0)
    slots = jnp.arange(cap, dtype=jnp.int32)
    place = jnp.where(slots[None, :] < counts[:, None], starts[:, None] + slots[None, :], -1)
    hit = place.reshape(-1)[None, :] == jnp.arange(total, dtype=jnp.int32)[:, None]
    row_targets = jnp.sum(jnp.where(hit, targets_all.reshape(-1)[None, :], 0), axis=1)

    rows = jnp.dot(hit.astype(bf16), gathered, preferred_element_type=f32).astype(bf16)
    parts = [rows[:, l * width_in : (l + 1) * width_in] for l in range(layers + 1)]
    in_pos = vocab_index * width_in + jnp.arange(width_in, dtype=jnp.int32)
    out_pos = seq_index * width_out + jnp.arange(width_out, dtype=jnp.int32)
    identity = (in_pos[:, None] == out_pos[None, :]).astype(bf16)
    bias = jnp.where(vocab_index == 0, translator_bias, 0.0)
    pieces = []
    for l in range(layers + 1):
        piece = jnp.dot(parts[l], identity, preferred_element_type=f32)
        if l < layers:
            piece = piece + jnp.dot(parts[l], translator[l], preferred_element_type=f32) + bias[l]
        pieces.append(piece)
    partial_value = jnp.concatenate(pieces, axis=0)
    lensed = lax.psum_scatter(partial_value, "vocab", scatter_dimension=0, tiled=True)
    squares = jnp.sum(lensed * lensed, axis=1)
    scaled = lax.all_gather(
        (lensed * norm_gain[None, :]).astype(bf16), "vocab", axis=0, tiled=True
    )
    chunk = stacked // vocab_count
    spread = jnp.where(
        jnp.arange(vocab_count, dtype=jnp.int32)[:, None] == vocab_index,
        squares.reshape(1, chunk),
        0.0,
    )
    every_square = lax.psum(lax.psum(spread, "vocab"), "seq").reshape(stacked)
    factor = lax.rsqrt(every_square / model + 1e-05)

    results = readout(
        scaled,
        factor.reshape(layers + 1, 1, total),
        row_targets.reshape(1, total),
        unembed,
        layers + 1,
        total,
        seq_count,
        vocab_count,
        model,
    )[: 2 * layers + 1]
    mine = lax.dynamic_slice_in_dim(place, seq_index, 1, axis=0)
    own = mine.reshape(cap, 1) == jnp.arange(total, dtype=jnp.int32)[None, :]
    out = jnp.sum(jnp.where(own[None], results[:, None, :], 0.0), axis=2)
    return (out[: layers + 1, None, :], out[layers + 1 :, None, :])


def solution(mesh):
    in_specs = (
        P(None, "seq", "vocab"),
        P("seq", "vocab"),
        P(None, "vocab", "seq"),
        P(None, "seq"),
        P("seq"),
        P("vocab", "seq"),
        P("seq", None),
        P("seq"),
        P("seq", None),
    )
    out_specs = (P(None, "seq", None), P(None, "seq", None))
    return jax.shard_map(body, mesh=mesh, in_specs=in_specs, out_specs=out_specs, check_vma=False)
```

```python
import math
import jax
import jax.numpy as jnp
from jax import lax
from jax.experimental import pallas as pl
from jax.experimental.pallas import tpu as pltpu
from jax.sharding import PartitionSpec as P

FLAG_DEV = 16
STATE_MAX, MATRIX_MAX, BIAS_MAX, GAIN_MAX, UNEMBED_MAX = 6.0, 0.078125, 4.0, 1.5, 0.21875
CHUNKS = 4
LAG = 2
SLOTS = 4
LEAD = 3 * CHUNKS
MESH = pl.DeviceIdType.MESH
f32, bf16, i16, i32 = jnp.float32, jnp.bfloat16, jnp.int16, jnp.int32


class Code:
    def __init__(self, model):
        widest = GAIN_MAX * UNEMBED_MAX * model * (STATE_MAX + BIAS_MAX + model * STATE_MAX * MATRIX_MAX)
        self.knee = 7.5e-4
        self.scale = 32700.0 / math.log2(1.0 + 1.02 * widest / self.knee)

    def enc(self, value):
        level = jnp.log2(1.0 + jnp.abs(value) * (1.0 / self.knee)) * self.scale
        return jnp.round(jnp.where(value < 0, -level, level)).astype(i32).astype(i16)

    def dec(self, code):
        level = code.astype(i32).astype(f32)
        size = (jnp.exp2(jnp.abs(level) * (1.0 / self.scale)) - 1.0) * self.knee
        return jnp.where(level < 0, -size, size)


def kernel(
    layers, total, cap, seq_count, vocab_count, model, code,
    probed, final, meta, bias, gain, t_hbm, u_hbm, out_ref,
    u, tr, rows, packed, hit, tgt, spot_col, meta_recv, rs_src, rs_recv, y, sq_part, sq_src, sq_recv, fac,
    own, psend, precv, zsend, zrecv, z3, e3, acc, stat_send, stat_recv, line_send, line_recv,
    u_sem, t_sem, msend_sem, mrecv_sem, rsend_sem, rrecv_sem, fsend_sem, frecv_sem, gsend_sem, grecv_sem,
    ysend_sem, yrecv_sem, qsend_sem, qrecv_sem, vsend_sem, vrecv_sem,
    psend_sem, precv_sem, zsend_sem, zrecv_sem, ssend_sem, srecv_sem, lsend_sem, lrecv_sem,
):
    seq, voc = lax.axis_index("seq"), lax.axis_index("vocab")
    chip, core = seq // 2, seq % 2
    chips = seq_count // 2
    vp, wo = u.shape
    wi = final.shape[1]
    ratio = wi // wo
    half, quarter = vp // 2, vp // 4
    chunk = quarter // CHUNKS
    steps = layers * CHUNKS
    plane = 2 * vocab_count
    share = total // vocab_count
    me = core * vocab_count + voc
    at_end = jnp.logical_or(chip == 0, chip == chips - 1)
    holder = seq // ratio
    holds = holder == voc
    home = (voc * ratio) // 2
    at_home = chip == home

    pieces = 4 * CHUNKS
    piece = vp // pieces

    def u_copy(k):
        part = pl.ds(pl.multiple_of(k * piece, piece), piece)
        return pltpu.make_async_copy(u_hbm.at[part], u.at[part], u_sem.at[k])

    def t_copy(l):
        return pltpu.make_async_copy(t_hbm.at[l], tr.at[l], t_sem.at[l])

    def remote(src, dst, send, recv, device):
        return pltpu.make_async_remote_copy(
            src_ref=src, dst_ref=dst, send_sem=send, recv_sem=recv, device_id=device, device_id_type=MESH
        )

    @pl.loop(0, layers - 1)
    def _(l):
        t_copy(l).start()

    @pl.loop(0, pieces)
    def _(k):
        u_copy(k).start()

    barrier = pltpu.get_barrier_semaphore()

    def in_plane(p):
        q = lax.rem(me + p, plane)
        return q, (chip * 2 + q // vocab_count, lax.rem(q, vocab_count))

    def in_line(p):
        q = lax.rem(chip + p, chips)
        return q, (q * 2 + core, voc)

    def in_column(p):
        q = lax.rem(seq + p, seq_count)
        return q, (q, voc)

    def in_group(p):
        q = lax.rem(voc + p, vocab_count)
        return q, (seq, q)

    partner = (chip * 2 + 1 - core, voc)

    @pl.loop(1, plane)
    def _(p):
        pl.semaphore_signal(barrier, inc=1, device_id=in_plane(p)[1], device_id_type=MESH)

    @pl.loop(1, seq_count)
    def _(p):
        pl.semaphore_signal(barrier, inc=1, device_id=in_column(p)[1], device_id_type=MESH)

    pl.semaphore_wait(barrier, plane - 1 + seq_count - 1)

    def meta_copy(p, slot):
        return remote(meta, meta_recv.at[slot], msend_sem.at[p], mrecv_sem.at[slot], in_column(p)[1])

    @pl.loop(1, seq_count)
    def _(p):
        meta_copy(p, seq).start()

    meta_recv[seq] = meta[...]

    def block(s):
        return pl.ds(pl.multiple_of(s * cap, cap), cap)

    def row_src(i):
        return final if i == 0 else probed.at[i - 1]

    def row_copy(i, p, source):
        src = rows.at[i, block(seq)] if not isinstance(i, int) else row_src(i)
        q, there = in_line(p)
        return remote(
            src, rows.at[i, block(source * 2 + core)], rsend_sem.at[i, p], rrecv_sem.at[i, source], there
        )

    def forward_copy(i, source, other, src=None):
        part = rows.at[i, block(source * 2 + (1 - core if other else core))]
        return remote(part if src is None else src, part, fsend_sem.at[i, source], frecv_sem.at[i, source], partner)

    for i in range(layers):
        if i == 0:
            @pl.loop(1, chips)
            def _(p):
                @pl.when(in_line(p)[0] == home)
                def _():
                    row_copy(0, p, chip).start()

            @pl.when(at_home)
            def _():
                forward_copy(0, chip, False, row_src(0)).start()
        else:
            @pl.loop(1, chips)
            def _(p):
                row_copy(i, p, chip).start()

            forward_copy(i, chip, False, row_src(i)).start()
        rows[i, block(seq), :] = row_src(i)[...]

    acc[...] = jnp.zeros_like(acc)

    def places():
        @pl.loop(1, seq_count)
        def _(p):
            q, _ = in_column(p)
            meta_copy(p, q).wait_recv()

        every = meta_recv[0]
        for q in range(1, seq_count):
            every = every + meta_recv[q]
        slots = seq_count * cap
        lane = lax.broadcasted_iota(i32, (1, slots), 1)
        counts, wanted, starts = every[0:1], every[1:2], every[2:3]
        slot = lane % cap
        place = jnp.where(slot < counts, starts + slot, -1)
        match = (lax.broadcasted_iota(i32, (total, slots), 0) == place).astype(f32).astype(bf16)
        hit[...] = match
        high = wanted // 256
        low = wanted - high * 256
        table = jnp.concatenate(
            [high.astype(f32), low.astype(f32), (place + 1).astype(f32), jnp.zeros((5, slots), f32)], axis=0
        ).astype(bf16)
        names = lax.dot_general(table, match, (((1,), (1,)), ((), ())), preferred_element_type=f32)
        tgt[...] = (names[0:1] * 256.0 + names[1:2]).astype(i32)
        mine = (
            lax.broadcasted_iota(i32, (cap, slots), 0) + seq * cap == lax.broadcasted_iota(i32, (cap, slots), 1)
        ).astype(f32).astype(bf16)
        spots = lax.dot_general(mine, table, (((1,), (1,)), ((), ())), preferred_element_type=f32)
        spot_col[...] = jnp.broadcast_to(spots[:, 2:3] - 1.0, spot_col.shape)

    def wants(i, then):
        pl.when(jnp.logical_or(i > 0, at_home))(then)

    def relay(i):
        def go():
            @pl.loop(1, chips)
            def _(p):
                q, _ = in_line(p)
                row_copy(i, p, q).wait_recv()
                forward_copy(i, q, False).start()

        wants(i, go)

    def part_of(q):
        return pl.ds(pl.multiple_of(q * share, share), share)

    def group_copy(i, p, slot):
        q, there = in_group(p)
        return remote(
            rs_src.at[i, part_of(q)], rs_recv.at[i, slot], gsend_sem.at[i, p], grecv_sem.at[i, slot], there
        )

    def translate(i):
        def go():
            @pl.loop(0, chips)
            def _(q):
                forward_copy(i, q, True).wait_recv()

            packed[...] = jnp.dot(hit[...], rows[i], preferred_element_type=f32).astype(bf16)

            @pl.when(i > 0)
            def _():
                t_copy(i - 1).wait()
                rs_src[i] = jnp.dot(packed[...], tr[i - 1], preferred_element_type=f32)

            @pl.when(holds)
            def _():
                start = pl.multiple_of(lax.rem(seq, ratio) * wo, wo)
                kept = packed[:, pl.ds(start, wo)].astype(f32)

                @pl.when(i > 0)
                def _():
                    rs_src[i] = rs_src[i] + kept

                @pl.when(i == 0)
                def _():
                    rs_src[i] = kept

            @pl.when(jnp.logical_or(i > 0, holds))
            def _():
                @pl.loop(1, vocab_count)
                def _(p):
                    group_copy(i, p, voc).start()

                rs_recv[i, voc] = rs_src[i, part_of(voc), :]

        wants(i, go)

    def y_copy(i, p, owner):
        return remote(
            y.at[i, part_of(owner)], y.at[i, part_of(owner)], ysend_sem.at[i, p], yrecv_sem.at[i, owner],
            in_group(p)[1],
        )

    def sq_copy(i, p, owner):
        return remote(
            sq_part.at[i, owner], sq_part.at[i, owner], qsend_sem.at[i, p], qrecv_sem.at[i, owner], in_group(p)[1]
        )

    def scale(i):
        def go(x):
            y[i, part_of(voc), :] = (x * gain[...]).astype(bf16)
            column = jnp.sum(x * x, axis=1, keepdims=True)
            lane = lax.broadcasted_iota(i32, (share, total), 1)
            row = lax.broadcasted_iota(i32, (share, total), 0) + voc * share
            sq_part[i, voc] = jnp.sum(jnp.where(lane == row, column, 0.0), axis=0, keepdims=True)

            @pl.loop(1, vocab_count)
            def _(p):
                y_copy(i, p, voc).start()

            @pl.loop(1, vocab_count)
            def _(p):
                sq_copy(i, p, voc).start()

        @pl.when(i > 0)
        def _():
            @pl.loop(1, vocab_count)
            def _(p):
                q, _ = in_group(p)
                group_copy(i, p, q).wait_recv()

            x = rs_recv[i, 0]
            for q in range(1, vocab_count):
                x = x + rs_recv[i, q]
            go(x + bias[i - 1])

        @pl.when(i == 0)
        def _():
            @pl.when(jnp.logical_not(holds))
            def _():
                group_copy(0, 1, holder).wait_recv()

            go(rs_recv[0, holder])

    def end_device(e):
        return jnp.where(e < 2, 0, seq_count - 2) + lax.rem(e, 2)

    def v_copy(i, e, source):
        return remote(
            sq_src.at[i], sq_recv.at[i, source], vsend_sem.at[i, e], vrecv_sem.at[i, source], (end_device(e), voc)
        )

    def collect(i):
        @pl.loop(1, vocab_count)
        def _(p):
            q, _ = in_group(p)
            y_copy(i, p, q).wait_recv()
            sq_copy(i, p, q).wait_recv()

        sums = sq_part[i, 0]
        for q in range(1, vocab_count):
            sums = sums + sq_part[i, q]
        sq_src[i] = sums

        @pl.loop(0, 4)
        def _(e):
            @pl.when(end_device(e) != seq)
            def _():
                v_copy(i, e, seq).start()

        @pl.when(at_end)
        def _():
            sq_recv[i, seq] = sums

    def pair_copy(t):
        return remote(
            psend.at[lax.rem(t, SLOTS)], precv.at[t], psend_sem.at[lax.rem(t, SLOTS)], precv_sem.at[t], partner
        )

    def line_copy(k, d):
        to = jnp.minimum(chip + 1, chips - 1) if d == 0 else jnp.maximum(chip - 1, 0)
        return remote(
            zsend.at[k, d], zrecv.at[k, d], zsend_sem.at[k, d], zrecv_sem.at[k, d], (to * 2 + core, voc)
        )

    def rows_at(owner, d, j):
        start = owner * half + d * quarter + j * chunk
        return pl.ds(pl.multiple_of(start, chunk), chunk)

    def product(part, yl):
        return lax.dot_general(u[part, :], yl, (((1,), (1,)), ((), ())), preferred_element_type=f32)

    def fold(value):
        return jnp.sum(value.reshape(chunk // 8, 8, total), axis=0)

    def finish(k, d, value):
        i, j = k // CHUNKS, lax.rem(k, CHUNKS)

        @pl.when(j == 0)
        def _():
            @pl.loop(1, seq_count)
            def _(p):
                q, _ = in_column(p)
                v_copy(i, 0, q).wait_recv()

            squares = sq_recv[i, 0]
            for q in range(1, seq_count):
                squares = squares + sq_recv[i, q]
            fac[i] = lax.rsqrt(squares * (1.0 / model) + 1e-05)

        logit = value * fac[i]
        base = voc * vp + core * half + d * quarter + j * chunk
        spot = lax.broadcasted_iota(i32, (chunk, total), 0) + base
        grown = jnp.exp(logit)
        acc[i] += fold(grown)
        acc[layers + i] += fold(jnp.where(spot == tgt[...], logit, 0.0))

        @pl.when(i == 0)
        def _():
            z3[j] = logit
            e3[j] = grown

        @pl.when(i > 0)
        def _():
            acc[2 * layers + i] += fold(e3[j] * (z3[j] - logit))

    def forward(k, d):
        first = chip == (0 if d == 0 else chips - 1)
        last = chip == (chips - 1 if d == 0 else 0)

        @pl.when(jnp.logical_not(first))
        def _():
            line_copy(k, d).wait_recv()
            own[k, d] = own[k, d] + code.dec(zrecv[k, d])

        @pl.when(jnp.logical_not(last))
        def _():
            zsend[k, d] = code.enc(own[k, d])
            line_copy(k, d).start()

        @pl.when(last)
        def _():
            finish(k, d, own[k, d])

    def stage(t, turn, ahead, then):
        i = t // CHUNKS + ahead

        @pl.when(jnp.logical_and(lax.rem(t, CHUNKS) == turn, jnp.logical_and(i >= 0, i < layers)))
        def _():
            then(i)

    turns = [(CHUNKS * k) // 4 for k in range(4)]

    @pl.loop(LEAD - 2 * CHUNKS - (CHUNKS - turns[3]), LEAD + steps + 1 + LAG * (chips - 1))
    def _(now):
        t = now - LEAD
        stage(now, turns[0], -LEAD // CHUNKS, collect)
        stage(now, turns[3], 3 - LEAD // CHUNKS, relay)
        pl.when(t == turns[3] - 3 * CHUNKS)(places)
        stage(now, turns[1], 2 - LEAD // CHUNKS, translate)
        stage(now, turns[2], 1 - LEAD // CHUNKS, scale)

        @pl.when(jnp.logical_and(t >= 0, t < CHUNKS))
        def _():
            for part in range(4):
                u_copy(part * CHUNKS + t).wait()

        @pl.when(jnp.logical_and(t >= 0, t < steps))
        def _():
            i, j = t // CHUNKS, lax.rem(t, CHUNKS)
            yl = y[i]

            @pl.when(t >= SLOTS)
            def _():
                pair_copy(t - SLOTS).wait_send()

            for d in range(2):
                psend[lax.rem(t, SLOTS), d] = product(rows_at(1 - core, d, j), yl)
            pair_copy(t).start()
            for d in range(2):
                own[t, d] = product(rows_at(core, d, j), yl)

        @pl.when(jnp.logical_and(t >= 1, t <= steps))
        def _():
            pair_copy(t - 1).wait_recv()
            own[t - 1] = own[t - 1] + precv[t - 1]

        for d in range(2):
            k = t - 1 - LAG * (chip if d == 0 else chips - 1 - chip)

            @pl.when(jnp.logical_and(k >= 0, k < steps))
            def _():
                forward(k, d)

    def stat_copy(p, slot):
        return remote(stat_send, stat_recv.at[slot], ssend_sem.at[p], srecv_sem.at[slot], in_plane(p)[1])

    end = jnp.where(chip == 0, 0, 1)

    def line_stat(p, side):
        return remote(line_send, line_recv.at[side], lsend_sem.at[p], lrecv_sem.at[side], in_line(p)[1])

    @pl.when(at_end)
    def _():
        stat = jnp.concatenate(
            [jnp.sum(acc[i], axis=0, keepdims=True) for i in range(3 * layers)]
            + [jnp.zeros((stat_send.shape[0] - 3 * layers, total), f32)] * (stat_send.shape[0] > 3 * layers),
            axis=0,
        )
        stat_send[...] = stat
        stat_recv[me] = stat

        @pl.loop(1, plane)
        def _(p):
            stat_copy(p, me).start()

        @pl.loop(1, plane)
        def _(p):
            stat_copy(p, in_plane(p)[0]).wait_recv()

        full = stat_recv[0]
        for q in range(1, plane):
            full = full + stat_recv[q]
        line_send[...] = full
        line_recv[end] = full

        @pl.loop(1, chips)
        def _(p):
            line_stat(p, end).start()

    @pl.loop(1, seq_count)
    def _(p):
        meta_copy(p, seq).wait_send()

    @pl.loop(0, layers)
    def _(i):
        @pl.loop(1, chips)
        def _(p):
            @pl.when(jnp.logical_or(i > 0, in_line(p)[0] == home))
            def _():
                row_copy(i, p, chip).wait_send()

        @pl.when(jnp.logical_or(i > 0, at_home))
        def _():
            @pl.loop(0, chips)
            def _(q):
                forward_copy(i, q, False).wait_send()

        @pl.loop(1, vocab_count)
        def _(p):
            @pl.when(jnp.logical_or(i > 0, holds))
            def _():
                group_copy(i, p, voc).wait_send()

            y_copy(i, p, voc).wait_send()
            sq_copy(i, p, voc).wait_send()

        @pl.loop(0, 4)
        def _(e):
            @pl.when(end_device(e) != seq)
            def _():
                v_copy(i, e, seq).wait_send()

    @pl.loop(steps - SLOTS, steps)
    def _(t):
        pair_copy(t).wait_send()

    @pl.loop(0, steps)
    def _(k):
        for d in range(2):
            @pl.when(chip != (chips - 1 if d == 0 else 0))
            def _():
                line_copy(k, d).wait_send()

    @pl.when(at_end)
    def _():
        @pl.loop(1, plane)
        def _(p):
            stat_copy(p, me).wait_send()

        @pl.loop(1, chips)
        def _(p):
            line_stat(p, end).wait_send()

    for side in range(2):
        @pl.when(chip != (0 if side == 0 else chips - 1))
        def _():
            line_stat(1, side).wait_recv()

    full = line_recv[0] + line_recv[1]
    total_exp, picked = full[:layers], full[layers : 2 * layers]
    cross = full[2 * layers + 1 : 3 * layers]
    log_total = jnp.log(total_exp)
    result = [picked[l : l + 1] - log_total[l : l + 1] for l in list(range(1, layers)) + [0]]
    for l in range(1, layers):
        result.append(cross[l - 1 : l] / total_exp[0:1] - log_total[0:1] + log_total[l : l + 1])
    lane = lax.broadcasted_iota(i32, (cap, total), 1).astype(f32)
    owned = lane == spot_col[...]
    place = lax.broadcasted_iota(i32, out_ref.shape, 1)
    out = jnp.zeros(out_ref.shape, f32)
    for l, value in enumerate(result):
        column = jnp.sum(jnp.where(owned, value, 0.0), axis=1, keepdims=True)
        out = jnp.where(place == l, column, out)
    out_ref[...] = out


def readout(probed, final, meta, bias, gain, translator, unembed, seq_count, vocab_count, cap, total, model):
    layers = probed.shape[0] + 1
    vp, wo = unembed.shape
    wi = final.shape[1]
    steps = layers * CHUNKS
    chunk = vp // 4 // CHUNKS
    plane, chips = 2 * vocab_count, seq_count // 2
    share = total // vocab_count
    code = Code(model)
    deep = -(-3 * layers // 8) * 8
    dma = pltpu.SemaphoreType.DMA
    vmem = pl.BlockSpec(memory_space=pltpu.VMEM)
    hbm = pl.BlockSpec(memory_space=pl.ANY)
    body = lambda *refs: kernel(layers, total, cap, seq_count, vocab_count, model, code, *refs)
    return pl.pallas_call(
        body,
        out_shape=jax.ShapeDtypeStruct((cap, 128), f32),
        in_specs=[vmem] * 5 + [hbm, hbm],
        out_specs=vmem,
        scratch_shapes=[
            pltpu.VMEM((vp, wo), bf16),
            pltpu.VMEM((layers - 1, wi, wo), bf16),
            pltpu.VMEM((layers, seq_count * cap, wi), bf16),
            pltpu.VMEM((total, wi), bf16),
            pltpu.VMEM((total, seq_count * cap), bf16),
            pltpu.VMEM((1, total), i32),
            pltpu.VMEM((cap, total), f32),
            pltpu.VMEM((seq_count, 8, seq_count * cap), i32),
            pltpu.VMEM((layers, total, wo), f32),
            pltpu.VMEM((layers, vocab_count, share, wo), f32),
            pltpu.VMEM((layers, total, wo), bf16),
            pltpu.VMEM((layers, vocab_count, 1, total), f32),
            pltpu.VMEM((layers, 1, total), f32),
            pltpu.VMEM((layers, seq_count, 1, total), f32),
            pltpu.VMEM((layers, 1, total), f32),
            pltpu.VMEM((steps, 2, chunk, total), f32),
            pltpu.VMEM((SLOTS, 2, chunk, total), f32),
            pltpu.VMEM((steps, 2, chunk, total), f32),
            pltpu.VMEM((steps, 2, chunk, total), i16),
            pltpu.VMEM((steps, 2, chunk, total), i16),
            pltpu.VMEM((CHUNKS, chunk, total), f32),
            pltpu.VMEM((CHUNKS, chunk, total), f32),
            pltpu.VMEM((3 * layers, 8, total), f32),
            pltpu.VMEM((deep, total), f32),
            pltpu.VMEM((plane, deep, total), f32),
            pltpu.VMEM((deep, total), f32),
            pltpu.VMEM((2, deep, total), f32),
            dma((4 * CHUNKS,)),
            dma((layers - 1,)),
            dma((seq_count,)),
            dma((seq_count,)),
            dma((layers, chips)),
            dma((layers, chips)),
            dma((layers, chips)),
            dma((layers, chips)),
            dma((layers, vocab_count)),
            dma((layers, vocab_count)),
            dma((layers, vocab_count)),
            dma((layers, vocab_count)),
            dma((layers, vocab_count)),
            dma((layers, vocab_count)),
            dma((layers, 4)),
            dma((layers, seq_count)),
            dma((SLOTS,)),
            dma((steps,)),
            dma((steps, 2)),
            dma((steps, 2)),
            dma((plane,)),
            dma((plane,)),
            dma((chips,)),
            dma((2,)),
        ],
        compiler_params=pltpu.CompilerParams(
            collective_id=0, has_side_effects=True, vmem_limit_bytes=63 << 20
        ),
        name="readout",
    )(probed, final, meta, bias, gain, translator, unembed)


def body(
    probe_states,
    final_states,
    translator,
    translator_bias,
    norm_gain,
    unembed,
    answer_rows,
    answer_count,
    targets,
):
    seq_count = lax.axis_size("seq")
    vocab_count = lax.axis_size("vocab")
    seq_index = lax.axis_index("seq")
    layers = probe_states.shape[0]
    cap = answer_rows.shape[1]
    model = probe_states.shape[2] * vocab_count
    picks = answer_rows[0]

    probed = jnp.take(probe_states, picks, axis=1, mode="clip")
    final = jnp.take(final_states, picks, axis=0, mode="clip")
    lane = jnp.arange(seq_count * cap, dtype=i32)[None, :]
    line = jnp.arange(8, dtype=i32)[:, None]
    mine = lane // cap == seq_index
    after = lane // cap > seq_index
    meta = jnp.where(jnp.logical_and(line == 0, mine), answer_count[0], 0)
    meta = jnp.where(jnp.logical_and(line == 1, mine), jnp.tile(targets, (1, seq_count)), meta)
    meta = jnp.where(jnp.logical_and(line == 2, after), answer_count[0], meta)

    out = readout(
        probed,
        final,
        meta,
        translator_bias[:, None, :],
        norm_gain[None, :],
        translator,
        unembed,
        seq_count,
        vocab_count,
        cap,
        seq_count * FLAG_DEV,
        model,
    )
    flat = out[:, : 2 * layers + 1].T
    return (flat[: layers + 1, None, :], flat[layers + 1 :, None, :])


def solution(mesh):
    in_specs = (
        P(None, "seq", "vocab"),
        P("seq", "vocab"),
        P(None, "vocab", "seq"),
        P(None, "seq"),
        P("seq"),
        P("vocab", "seq"),
        P("seq", None),
        P("seq"),
        P("seq", None),
    )
    out_specs = (P(None, "seq", None), P(None, "seq", None))
    return jax.shard_map(body, mesh=mesh, in_specs=in_specs, out_specs=out_specs, check_vma=False)
```

```python
import math
import jax
import jax.numpy as jnp
from jax import lax
from jax.experimental import pallas as pl
from jax.experimental.pallas import tpu as pltpu
from jax.sharding import PartitionSpec as P

FLAG_DEV = 16
STATE_MAX, MATRIX_MAX, BIAS_MAX, GAIN_MAX, UNEMBED_MAX = 6.0, 0.078125, 4.0, 1.5, 0.21875
CHUNKS = 4
LAG = 2
SLOTS = 4
PACK = 8
LEAD = 3 * CHUNKS
MESH = pl.DeviceIdType.MESH
f32, bf16, i16, i32 = jnp.float32, jnp.bfloat16, jnp.int16, jnp.int32


class Code:
    def __init__(self, widest):
        self.knee = 7.5e-4
        self.scale = 32700.0 / math.log2(1.0 + 1.02 * widest / self.knee)

    def enc(self, value):
        level = jnp.log2(1.0 + jnp.abs(value) * (1.0 / self.knee)) * self.scale
        return jnp.round(jnp.where(value < 0, -level, level)).astype(i32).astype(i16)

    def dec(self, code):
        level = code.astype(i32).astype(f32)
        size = (jnp.exp2(jnp.abs(level) * (1.0 / self.scale)) - 1.0) * self.knee
        return jnp.where(level < 0, -size, size)


def kernel(
    layers, total, cap, seq_count, vocab_count, model, code, xcode,
    picked_rows, count, wanted_ref, bias, gain, t_hbm, u_hbm, prob_ref, kl_ref,
    u, tr, meta, rows, packed, hit, tgt, spot_col, meta_recv, part, rs_own, rs_src, rs_recv, y, sq_part, sq_src, sq_recv, fac,
    own, psend, precv, zsend, zrecv, z3, e3, acc, stat_send, stat_recv, line_send, line_recv,
    u_sem, t_sem, msend_sem, mrecv_sem, rsend_sem, rrecv_sem, fsend_sem, frecv_sem, gsend_sem, grecv_sem,
    ysend_sem, yrecv_sem, qsend_sem, qrecv_sem, vsend_sem, vrecv_sem,
    psend_sem, precv_sem, zsend_sem, zrecv_sem, ssend_sem, srecv_sem, lsend_sem, lrecv_sem,
):
    seq, voc = lax.axis_index("seq"), lax.axis_index("vocab")
    chip, core = seq // 2, seq % 2
    chips = seq_count // 2
    vp, wo = u.shape
    wi = picked_rows.shape[2]
    ratio = wi // wo
    half, quarter = vp // 2, vp // 4
    chunk = quarter // CHUNKS
    steps = layers * CHUNKS
    plane = 2 * vocab_count
    share = total // vocab_count
    me = core * vocab_count + voc
    at_end = jnp.logical_or(chip == 0, chip == chips - 1)
    holder = seq // ratio
    holds = holder == voc
    home = (voc * ratio) // 2
    at_home = chip == home

    pieces = 4 * CHUNKS
    piece = vp // pieces

    def u_copy(k):
        part = pl.ds(pl.multiple_of(k * piece, piece), piece)
        return pltpu.make_async_copy(u_hbm.at[part], u.at[part], u_sem.at[k])

    def t_copy(l):
        return pltpu.make_async_copy(t_hbm.at[l], tr.at[l], t_sem.at[l])

    def remote(src, dst, send, recv, device):
        return pltpu.make_async_remote_copy(
            src_ref=src, dst_ref=dst, send_sem=send, recv_sem=recv, device_id=device, device_id_type=MESH
        )

    meta[...] = jnp.full(meta.shape, count[0], i32)
    meta[:, :cap] = wanted_ref[...]

    @pl.loop(0, layers - 1)
    def _(l):
        t_copy(l).start()

    @pl.loop(0, pieces)
    def _(k):
        u_copy(k).start()

    barrier = pltpu.get_barrier_semaphore()

    def in_plane(p):
        q = lax.rem(me + p, plane)
        return q, (chip * 2 + q // vocab_count, lax.rem(q, vocab_count))

    def in_line(p):
        q = lax.rem(chip + p, chips)
        return q, (q * 2 + core, voc)

    def in_column(p):
        q = lax.rem(seq + p, seq_count)
        return q, (q, voc)

    def in_group(p):
        q = lax.rem(voc + p, vocab_count)
        return q, (seq, q)

    partner = (chip * 2 + 1 - core, voc)

    @pl.loop(1, plane)
    def _(p):
        pl.semaphore_signal(barrier, inc=1, device_id=in_plane(p)[1], device_id_type=MESH)

    @pl.loop(1, seq_count)
    def _(p):
        pl.semaphore_signal(barrier, inc=1, device_id=in_column(p)[1], device_id_type=MESH)

    with jax.named_scope('barrier'):
        pl.semaphore_wait(barrier, plane - 1 + seq_count - 1)

    def meta_copy(p, slot):
        return remote(meta, meta_recv.at[slot], msend_sem.at[p], mrecv_sem.at[slot], in_column(p)[1])

    @pl.loop(1, seq_count)
    def _(p):
        meta_copy(p, seq).start()

    meta_recv[seq] = meta[...]

    def block(s):
        return pl.ds(pl.multiple_of(s * cap, cap), cap)

    def row_src(i):
        return picked_rows.at[i]

    def row_copy(i, source, d, src=None):
        to = jnp.minimum(chip + 1, chips - 1) if d == 0 else jnp.maximum(chip - 1, 0)
        here = rows.at[i, block(source * 2 + core)]
        return remote(
            here if src is None else src, here, rsend_sem.at[i, source, d], rrecv_sem.at[i, source], (to * 2 + core, voc)
        )

    def passes(d):
        return chip < chips - 1 if d == 0 else chip > 0

    def home_copy(source):
        here = rows.at[0, block(source * 2 + core)]
        return remote(picked_rows.at[0], here, rsend_sem.at[0, chip, 0], rrecv_sem.at[0, source], (home * 2 + core, voc))

    def forward_copy(i, source, other, src=None):
        part = rows.at[i, block(source * 2 + (1 - core if other else core))]
        return remote(part if src is None else src, part, fsend_sem.at[i, source], frecv_sem.at[i, source], partner)

    def depart(i):
        for d in range(2):
            @pl.when(passes(d))
            def _():
                row_copy(i, chip, d, row_src(i)).start()

        forward_copy(i, chip, False, row_src(i)).start()

    @pl.when(at_home)
    def _():
        forward_copy(0, chip, False, picked_rows.at[0]).start()

    @pl.when(jnp.logical_not(at_home))
    def _():
        home_copy(chip).start()

    for i in range(layers):
        rows[i, block(seq), :] = row_src(i)[...]

    @pl.when(jnp.logical_not(at_home))
    def _():
        home_copy(chip).wait_send()

    depart(1)
    acc[...] = jnp.zeros_like(acc)

    def places():
        @pl.loop(1, seq_count)
        def _(p):
            q, _ = in_column(p)
            meta_copy(p, q).wait_recv()

        every = jnp.concatenate([meta_recv[q] for q in range(seq_count)], axis=0)
        slots = seq_count * cap
        lane = lax.broadcasted_iota(i32, (1, slots), 1)
        owner = lax.broadcasted_iota(i32, (seq_count, slots), 1) // cap
        row = lax.broadcasted_iota(i32, (seq_count, slots), 0)
        counted = jnp.broadcast_to(every[:, cap : cap + 1], (seq_count, slots))
        counts = jnp.sum(jnp.where(row == owner, counted, 0), axis=0, keepdims=True)
        starts = jnp.sum(jnp.where(row < owner, counted, 0), axis=0, keepdims=True)
        wide = every.shape[1]
        spread = (
            lax.broadcasted_iota(i32, (wide, slots), 0) == lax.broadcasted_iota(i32, (wide, slots), 1) % cap
        ).astype(f32).astype(bf16)
        high = every // 256
        low = every - high * 256

        def lanes(byte):
            laid = jnp.dot(byte.astype(f32).astype(bf16), spread, preferred_element_type=f32)
            return jnp.sum(jnp.where(row == owner, laid, 0.0), axis=0, keepdims=True)

        slot = lane % cap
        place = jnp.where(slot < counts, starts + slot, -1)
        match = (lax.broadcasted_iota(i32, (total, slots), 0) == place).astype(f32).astype(bf16)
        hit[...] = match
        table = jnp.concatenate(
            [lanes(high), lanes(low), (place + 1).astype(f32), jnp.zeros((5, slots), f32)], axis=0
        ).astype(bf16)
        names = lax.dot_general(table, match, (((1,), (1,)), ((), ())), preferred_element_type=f32)
        tgt[...] = (names[0:1] * 256.0 + names[1:2]).astype(i32)
        mine = (
            lax.broadcasted_iota(i32, (cap, slots), 0) + seq * cap == lax.broadcasted_iota(i32, (cap, slots), 1)
        ).astype(f32).astype(bf16)
        spots = lax.dot_general(mine, table, (((1,), (1,)), ((), ())), preferred_element_type=f32)
        spot_col[...] = jnp.broadcast_to(spots[:, 2:3] - 1.0, spot_col.shape)

    def wants(i, then):
        pl.when(jnp.logical_or(i > 0, at_home))(then)

    def gather_home():
        @pl.loop(1, chips)
        def _(p):
            q, _ = in_line(p)
            home_copy(q).wait_recv()
            forward_copy(0, q, False).start()

    def relay(i):
        @pl.loop(1, chips)
        def _(p):
            for d in range(2):
                source = chip - p if d == 0 else chip + p

                @pl.when(source >= 0 if d == 0 else source < chips)
                def _():
                    row_copy(i, source, d).wait_recv()

                    @pl.when(passes(d))
                    def _():
                        row_copy(i, source, d).start()

                    forward_copy(i, source, False).start()

    def early(i):
        pl.when(jnp.logical_and(i == 0, at_home))(gather_home)

        @pl.when(jnp.logical_and(i > 0, jnp.logical_not(at_end)))
        def _():
            relay(i)

        for later in range(2, layers):
            pl.when(i == later - 2)(lambda: depart(later))

    def late(i):
        @pl.when(jnp.logical_and(i > 0, at_end))
        def _():
            relay(i)

    def part_of(q):
        return pl.ds(pl.multiple_of(q * share, share), share)

    def group_copy(i, p, slot):
        q, there = in_group(p)
        return remote(
            rs_src.at[i, part_of(q)], rs_recv.at[i, slot], gsend_sem.at[i, p], grecv_sem.at[i, slot], there
        )

    def translate(i):
        def go():
            @pl.loop(0, chips)
            def _(q):
                forward_copy(i, q, True).wait_recv()

            packed[...] = jnp.dot(hit[...], rows[i], preferred_element_type=f32).astype(bf16)

            @pl.when(i > 0)
            def _():
                t_copy(i - 1).wait()
                part[...] = jnp.dot(packed[...], tr[i - 1], preferred_element_type=f32)

            @pl.when(holds)
            def _():
                start = pl.multiple_of(lax.rem(seq, ratio) * wo, wo)
                kept = packed[:, pl.ds(start, wo)].astype(f32)

                @pl.when(i > 0)
                def _():
                    part[...] = part[...] + kept

                @pl.when(i == 0)
                def _():
                    part[...] = kept

            @pl.when(jnp.logical_or(i > 0, holds))
            def _():
                rs_src[i] = xcode.enc(part[...])

                @pl.loop(1, vocab_count)
                def _(p):
                    group_copy(i, p, voc).start()

                rs_own[i] = part[part_of(voc), :]

        wants(i, go)

    def y_copy(i, p, owner):
        return remote(
            y.at[i, part_of(owner)], y.at[i, part_of(owner)], ysend_sem.at[i, p], yrecv_sem.at[i, owner],
            in_group(p)[1],
        )

    def sq_copy(i, p, owner):
        return remote(
            sq_part.at[i, owner], sq_part.at[i, owner], qsend_sem.at[i, p], qrecv_sem.at[i, owner], in_group(p)[1]
        )

    def scale(i):
        def go(x):
            y[i, part_of(voc), :] = (x * gain[...].reshape(1, wo)).astype(bf16)
            column = jnp.sum(x * x, axis=1, keepdims=True)
            lane = lax.broadcasted_iota(i32, (share, total), 1)
            row = lax.broadcasted_iota(i32, (share, total), 0) + voc * share
            sq_part[i, voc] = jnp.sum(jnp.where(lane == row, column, 0.0), axis=0, keepdims=True)

            @pl.loop(1, vocab_count)
            def _(p):
                y_copy(i, p, voc).start()

            @pl.loop(1, vocab_count)
            def _(p):
                sq_copy(i, p, voc).start()

        @pl.when(i > 0)
        def _():
            x = rs_own[i] + bias[pl.ds(i - 1, 1), :]
            for p in range(1, vocab_count):
                q, _ = in_group(p)
                group_copy(i, p, q).wait_recv()
                x = x + xcode.dec(rs_recv[i, q])
            go(x)

        @pl.when(jnp.logical_and(i == 0, holds))
        def _():
            go(rs_own[0])

        @pl.when(jnp.logical_and(i == 0, jnp.logical_not(holds)))
        def _():
            group_copy(0, 1, holder).wait_recv()
            go(xcode.dec(rs_recv[0, holder]))

    def end_device(e):
        return jnp.where(e < 2, 0, seq_count - 2) + lax.rem(e, 2)

    def v_copy(i, e, source):
        return remote(
            sq_src.at[i], sq_recv.at[i, source], vsend_sem.at[i, e], vrecv_sem.at[i, source], (end_device(e), voc)
        )

    def collect(i):
        @pl.loop(1, vocab_count)
        def _(p):
            q, _ = in_group(p)
            y_copy(i, p, q).wait_recv()
            sq_copy(i, p, q).wait_recv()

        sums = sq_part[i, 0]
        for q in range(1, vocab_count):
            sums = sums + sq_part[i, q]
        sq_src[i] = sums

        @pl.loop(0, 4)
        def _(e):
            @pl.when(end_device(e) != seq)
            def _():
                v_copy(i, e, seq).start()

        @pl.when(at_end)
        def _():
            sq_recv[i, seq] = sums

    def pair_copy(t):
        return remote(
            psend.at[lax.rem(t, SLOTS)], precv.at[t], psend_sem.at[lax.rem(t, SLOTS)], precv_sem.at[t], partner
        )

    def line_copy(k, d):
        to = jnp.minimum(chip + 1, chips - 1) if d == 0 else jnp.maximum(chip - 1, 0)
        return remote(
            zsend.at[k, d], zrecv.at[k, d], zsend_sem.at[k, d], zrecv_sem.at[k, d], (to * 2 + core, voc)
        )

    def rows_at(owner, d, j):
        start = owner * half + d * quarter + j * chunk
        return pl.ds(pl.multiple_of(start, chunk), chunk)

    def product(part, yl):
        return lax.dot_general(u[part, :], yl, (((1,), (1,)), ((), ())), preferred_element_type=f32)

    def fold(value):
        return jnp.sum(value.reshape(chunk // 8, 8, total), axis=0)

    def finish(k, d, value):
        i, j = k // CHUNKS, lax.rem(k, CHUNKS)

        @pl.when(j == 0)
        def _():
            @pl.loop(1, seq_count)
            def _(p):
                q, _ = in_column(p)
                v_copy(i, 0, q).wait_recv()

            squares = sq_recv[i, 0]
            for q in range(1, seq_count):
                squares = squares + sq_recv[i, q]
            fac[i] = lax.rsqrt(squares * (1.0 / model) + 1e-05)

        logit = value * fac[i]
        base = voc * vp + core * half + d * quarter + j * chunk
        spot = lax.broadcasted_iota(i32, (chunk, total), 0) + base
        grown = jnp.exp(logit)
        acc[i] += fold(grown)
        acc[layers + i] += fold(jnp.where(spot == tgt[...], logit, 0.0))

        @pl.when(i == 0)
        def _():
            z3[j] = logit
            e3[j] = grown

        @pl.when(i > 0)
        def _():
            acc[2 * layers + i] += fold(e3[j] * (z3[j] - logit))

    def forward(k, d):
        first = chip == (0 if d == 0 else chips - 1)
        last = chip == (chips - 1 if d == 0 else 0)

        @pl.when(jnp.logical_not(first))
        def _():
            with jax.named_scope('linewait'):
                line_copy(k, d).wait_recv()
            own[k, d] = own[k, d] + code.dec(zrecv[k, d])

        @pl.when(jnp.logical_not(last))
        def _():
            zsend[k, d] = code.enc(own[k, d])
            line_copy(k, d).start()

        @pl.when(last)
        def _():
            finish(k, d, own[k, d])

    def stage(t, turn, ahead, then):
        i = t // CHUNKS + ahead

        @pl.when(jnp.logical_and(lax.rem(t, CHUNKS) == turn, jnp.logical_and(i >= 0, i < layers)))
        def _():
            with jax.named_scope(then.__name__):
                then(i)

    turns = [(CHUNKS * k) // 4 for k in range(4)]

    @pl.loop(LEAD - 2 * CHUNKS - (CHUNKS - turns[3]), LEAD + steps + 1 + LAG * (chips - 1))
    def _(now):
        t = now - LEAD
        stage(now, turns[0], -LEAD // CHUNKS, collect)
        stage(now, turns[3], 3 - LEAD // CHUNKS, early)
        pl.when(t == turns[3] - 3 * CHUNKS)(places)
        stage(now, turns[1], 1 - LEAD // CHUNKS, scale)
        stage(now, turns[2], 2 - LEAD // CHUNKS, late)
        stage(now, turns[2], 2 - LEAD // CHUNKS, translate)

        @pl.when(jnp.logical_and(t >= 0, t < CHUNKS))
        def _():
            for part in range(4):
                u_copy(part * CHUNKS + t).wait()

        @pl.when(jnp.logical_and(t >= 0, t < steps))
        def _():
            i, j = t // CHUNKS, lax.rem(t, CHUNKS)
            yl = y[i]
            scope = jax.named_scope('dots'); scope.__enter__()

            @pl.when(t >= SLOTS)
            def _():
                pair_copy(t - SLOTS).wait_send()

            for d in range(2):
                psend[lax.rem(t, SLOTS), d] = product(rows_at(1 - core, d, j), yl)
            pair_copy(t).start()
            for d in range(2):
                own[t, d] = product(rows_at(core, d, j), yl)
            scope.__exit__(None, None, None)

        @pl.when(jnp.logical_and(t >= 1, t <= steps))
        def _():
            with jax.named_scope('pairsum'):
                pair_copy(t - 1).wait_recv()
                own[t - 1] = own[t - 1] + precv[t - 1]

        for d in range(2):
            k = t - 1 - LAG * (chip if d == 0 else chips - 1 - chip)

            @pl.when(jnp.logical_and(k >= 0, k < steps))
            def _():
                with jax.named_scope('fwd%d' % d):
                    forward(k, d)

    def stat_copy(p, slot):
        return remote(stat_send, stat_recv.at[slot], ssend_sem.at[p], srecv_sem.at[slot], in_plane(p)[1])

    end = jnp.where(chip == 0, 0, 1)

    def line_stat(p, side):
        return remote(line_send, line_recv.at[side], lsend_sem.at[p], lrecv_sem.at[side], in_line(p)[1])

    @pl.when(at_end)
    def _():
        stat = jnp.concatenate(
            [jnp.sum(acc[i], axis=0, keepdims=True) for i in range(3 * layers)]
            + [jnp.zeros((stat_send.shape[0] - 3 * layers, total), f32)] * (stat_send.shape[0] > 3 * layers),
            axis=0,
        )
        stat_send[...] = stat
        stat_recv[me] = stat

        @pl.loop(1, plane)
        def _(p):
            stat_copy(p, me).start()

        with jax.named_scope('planewait'):
            @pl.loop(1, plane)
            def _(p):
                stat_copy(p, in_plane(p)[0]).wait_recv()

        full = stat_recv[0]
        for q in range(1, plane):
            full = full + stat_recv[q]
        line_send[...] = full
        line_recv[end] = full

        @pl.loop(1, chips)
        def _(p):
            line_stat(p, end).start()

    @pl.loop(1, seq_count)
    def _(p):
        meta_copy(p, seq).wait_send()

    @pl.loop(0, layers)
    def _(i):
        @pl.loop(0, chips)
        def _(q):
            for d in range(2):
                @pl.when(jnp.logical_and(jnp.logical_and(i > 0, passes(d)), q <= chip if d == 0 else q >= chip))
                def _():
                    row_copy(i, q, d).wait_send()

        @pl.when(jnp.logical_or(i > 0, at_home))
        def _():
            @pl.loop(0, chips)
            def _(q):
                forward_copy(i, q, False).wait_send()

        @pl.loop(1, vocab_count)
        def _(p):
            @pl.when(jnp.logical_or(i > 0, holds))
            def _():
                group_copy(i, p, voc).wait_send()

            y_copy(i, p, voc).wait_send()
            sq_copy(i, p, voc).wait_send()

        @pl.loop(0, 4)
        def _(e):
            @pl.when(end_device(e) != seq)
            def _():
                v_copy(i, e, seq).wait_send()

    @pl.loop(steps - SLOTS, steps)
    def _(t):
        pair_copy(t).wait_send()

    @pl.loop(0, steps)
    def _(k):
        for d in range(2):
            @pl.when(chip != (chips - 1 if d == 0 else 0))
            def _():
                line_copy(k, d).wait_send()

    @pl.when(at_end)
    def _():
        @pl.loop(1, plane)
        def _(p):
            stat_copy(p, me).wait_send()

        @pl.loop(1, chips)
        def _(p):
            line_stat(p, end).wait_send()

    for side in range(2):
        @pl.when(chip != (0 if side == 0 else chips - 1))
        def _():
            with jax.named_scope('statwait'):
                line_stat(1, side).wait_recv()

    scope2 = jax.named_scope('final'); scope2.__enter__()
    full = line_recv[0] + line_recv[1]
    total_exp, picked = full[:layers], full[layers : 2 * layers]
    cross = full[2 * layers + 1 : 3 * layers]
    log_total = jnp.log(total_exp)
    result = [picked[l : l + 1] - log_total[l : l + 1] for l in list(range(1, layers)) + [0]]
    for l in range(1, layers):
        result.append(cross[l - 1 : l] / total_exp[0:1] - log_total[0:1] + log_total[l : l + 1])
    lane = lax.broadcasted_iota(i32, (cap, total), 1).astype(f32)
    owned = lane == spot_col[...]
    place = lax.broadcasted_iota(i32, (cap, 128), 1)
    out = jnp.zeros((cap, 128), f32)
    for l, value in enumerate(result):
        column = jnp.sum(jnp.where(owned, value, 0.0), axis=1, keepdims=True)
        out = jnp.where(place == l, column, out)
    turned = out.T
    for l in range(layers):
        prob_ref[l] = turned[l : l + 1]
    for l in range(layers - 1):
        kl_ref[l] = turned[layers + l : layers + l + 1]
    scope2.__exit__(None, None, None)


def pick_kernel(layers, cap, picks, probe_hbm, final_hbm, out_ref, found, sem):
    @pl.loop(0, cap)
    def _(k):
        first = pl.ds(pl.multiple_of(picks[0, k] // PACK * PACK, PACK), PACK)
        spot = pl.ds(pl.multiple_of(k * PACK, PACK), PACK)
        pltpu.make_async_copy(final_hbm.at[first], found.at[0, spot], sem.at[0]).start()
        for l in range(1, layers):
            pltpu.make_async_copy(probe_hbm.at[l - 1, first], found.at[l, spot], sem.at[l]).start()

    row = lax.broadcasted_iota(i32, (cap, cap * PACK), 0)
    wants = jnp.zeros((cap, cap * PACK), i32)
    for k in range(cap):
        wants = jnp.where(row == k, k * PACK + picks[0, k] % PACK, wants)
    match = (lax.broadcasted_iota(i32, (cap, cap * PACK), 1) == wants).astype(f32).astype(bf16)
    for l in range(layers):
        pltpu.make_async_copy(found.at[l], found.at[l], sem.at[l]).wait()
        out_ref[l] = jnp.dot(match, found[l], preferred_element_type=f32).astype(bf16)


def pick(answer_rows, probe_states, final_states):
    layers, cap, wi = probe_states.shape[0] + 1, answer_rows.shape[1], final_states.shape[1]
    hbm = pl.BlockSpec(memory_space=pl.ANY)
    return pl.pallas_call(
        lambda *refs: pick_kernel(layers, cap, *refs),
        out_shape=jax.ShapeDtypeStruct((layers, cap, wi), bf16),
        in_specs=[pl.BlockSpec(memory_space=pltpu.SMEM), hbm, hbm],
        out_specs=pl.BlockSpec(memory_space=pltpu.VMEM),
        scratch_shapes=[pltpu.VMEM((layers, cap * PACK, wi), bf16), pltpu.SemaphoreType.DMA((layers,))],
        name="pick",
    )(answer_rows, probe_states, final_states)


def readout(rows, count, wanted, bias, gain, translator, unembed, seq_count, vocab_count, total, model):
    layers, cap, wi = rows.shape
    vp, wo = unembed.shape
    steps = layers * CHUNKS
    chunk = vp // 4 // CHUNKS
    plane, chips = 2 * vocab_count, seq_count // 2
    share = total // vocab_count
    code = Code(GAIN_MAX * UNEMBED_MAX * model * (STATE_MAX + BIAS_MAX + model * STATE_MAX * MATRIX_MAX))
    xcode = Code(STATE_MAX + BIAS_MAX + model * STATE_MAX * MATRIX_MAX)
    deep = -(-3 * layers // 8) * 8
    dma = pltpu.SemaphoreType.DMA
    vmem = pl.BlockSpec(memory_space=pltpu.VMEM)
    hbm = pl.BlockSpec(memory_space=pl.ANY)
    body = lambda *refs: kernel(layers, total, cap, seq_count, vocab_count, model, code, xcode, *refs)
    return pl.pallas_call(
        body,
        out_shape=(
            jax.ShapeDtypeStruct((layers, 1, cap), f32),
            jax.ShapeDtypeStruct((layers - 1, 1, cap), f32),
        ),
        in_specs=[vmem, pl.BlockSpec(memory_space=pltpu.SMEM), vmem, vmem, vmem, hbm, hbm],
        out_specs=(vmem, vmem),
        scratch_shapes=[
            pltpu.VMEM((vp, wo), bf16),
            pltpu.VMEM((layers - 1, wi, wo), bf16),
            pltpu.VMEM((1, 128), i32),
            pltpu.VMEM((layers, seq_count * cap, wi), bf16),
            pltpu.VMEM((total, wi), bf16),
            pltpu.VMEM((total, seq_count * cap), bf16),
            pltpu.VMEM((1, total), i32),
            pltpu.VMEM((cap, total), f32),
            pltpu.VMEM((seq_count, 1, 128), i32),
            pltpu.VMEM((total, wo), f32),
            pltpu.VMEM((layers, share, wo), f32),
            pltpu.VMEM((layers, total, wo), i16),
            pltpu.VMEM((layers, vocab_count, share, wo), i16),
            pltpu.VMEM((layers, total, wo), bf16),
            pltpu.VMEM((layers, vocab_count, 1, total), f32),
            pltpu.VMEM((layers, 1, total), f32),
            pltpu.VMEM((layers, seq_count, 1, total), f32),
            pltpu.VMEM((layers, 1, total), f32),
            pltpu.VMEM((steps, 2, chunk, total), f32),
            pltpu.VMEM((SLOTS, 2, chunk, total), f32),
            pltpu.VMEM((steps, 2, chunk, total), f32),
            pltpu.VMEM((steps, 2, chunk, total), i16),
            pltpu.VMEM((steps, 2, chunk, total), i16),
            pltpu.VMEM((CHUNKS, chunk, total), f32),
            pltpu.VMEM((CHUNKS, chunk, total), f32),
            pltpu.VMEM((3 * layers, 8, total), f32),
            pltpu.VMEM((deep, total), f32),
            pltpu.VMEM((plane, deep, total), f32),
            pltpu.VMEM((deep, total), f32),
            pltpu.VMEM((2, deep, total), f32),
            dma((4 * CHUNKS,)),
            dma((layers - 1,)),
            dma((seq_count,)),
            dma((seq_count,)),
            dma((layers, chips, 2)),
            dma((layers, chips)),
            dma((layers, chips)),
            dma((layers, chips)),
            dma((layers, vocab_count)),
            dma((layers, vocab_count)),
            dma((layers, vocab_count)),
            dma((layers, vocab_count)),
            dma((layers, vocab_count)),
            dma((layers, vocab_count)),
            dma((layers, 4)),
            dma((layers, seq_count)),
            dma((SLOTS,)),
            dma((steps,)),
            dma((steps, 2)),
            dma((steps, 2)),
            dma((plane,)),
            dma((plane,)),
            dma((chips,)),
            dma((2,)),
        ],
        compiler_params=pltpu.CompilerParams(
            collective_id=0, has_side_effects=True, vmem_limit_bytes=63 << 20
        ),
        name="readout",
    )(rows, count, wanted, bias, gain, translator, unembed)


def body(
    probe_states,
    final_states,
    translator,
    translator_bias,
    norm_gain,
    unembed,
    answer_rows,
    answer_count,
    targets,
):
    seq_count = lax.axis_size("seq")
    vocab_count = lax.axis_size("vocab")
    model = probe_states.shape[2] * vocab_count
    return readout(
        pick(answer_rows, probe_states, final_states),
        answer_count,
        targets,
        translator_bias,
        norm_gain,
        translator,
        unembed,
        seq_count,
        vocab_count,
        seq_count * FLAG_DEV,
        model,
    )


def solution(mesh):
    in_specs = (
        P(None, "seq", "vocab"),
        P("seq", "vocab"),
        P(None, "vocab", "seq"),
        P(None, "seq"),
        P("seq"),
        P("vocab", "seq"),
        P("seq", None),
        P("seq"),
        P("seq", None),
    )
    out_specs = (P(None, "seq", None), P(None, "seq", None))
    return jax.shard_map(body, mesh=mesh, in_specs=in_specs, out_specs=out_specs, check_vma=False)
```

```python
import math
import jax
import jax.numpy as jnp
from jax import lax
from jax.experimental import pallas as pl
from jax.experimental.pallas import tpu as pltpu
from jax.sharding import PartitionSpec as P

FLAG_DEV = 16
STATE_MAX, MATRIX_MAX, BIAS_MAX, GAIN_MAX, UNEMBED_MAX = 6.0, 0.078125, 4.0, 1.5, 0.21875
CHUNKS = 4
LAG = 2
SLOTS = 4
PACK = 8
LEAD = 3 * CHUNKS
MESH = pl.DeviceIdType.MESH
f32, bf16, i16, i32 = jnp.float32, jnp.bfloat16, jnp.int16, jnp.int32

class Code:
    def __init__(self, widest):
        self.knee = 7.5e-4
        self.scale = 32700.0 / math.log2(1.0 + 1.02 * widest / self.knee)

    def enc(self, value):
        level = jnp.log2(1.0 + jnp.abs(value) * (1.0 / self.knee)) * self.scale
        return jnp.round(jnp.where(value < 0, -level, level)).astype(i32).astype(i16)

    def dec(self, code):
        level = code.astype(i32).astype(f32)
        size = (jnp.exp2(jnp.abs(level) * (1.0 / self.scale)) - 1.0) * self.knee
        return jnp.where(level < 0, -size, size)

def kernel(
    layers, total, cap, seq_count, vocab_count, model, code, xcode,
    picked_rows, count, wanted_ref, bias, gain, t_hbm, u_hbm, prob_ref, kl_ref,
    u, tr, meta, rows, packed, hit, tgt, spot_col, meta_recv, part, rs_own, rs_src, rs_recv, y, sq_part, sq_src, sq_recv, fac,
    own, psend, precv, zsend, zrecv, z3, e3, acc, stat_send, stat_recv, line_send, line_recv,
    u_sem, t_sem, msend_sem, mrecv_sem, rsend_sem, rrecv_sem, fsend_sem, frecv_sem, gsend_sem, grecv_sem,
    ysend_sem, yrecv_sem, qsend_sem, qrecv_sem, vsend_sem, vrecv_sem,
    psend_sem, precv_sem, zsend_sem, zrecv_sem, ssend_sem, srecv_sem, lsend_sem, lrecv_sem,
):
    seq, voc = lax.axis_index("seq"), lax.axis_index("vocab")
    chip, core = seq // 2, seq % 2
    chips = seq_count // 2
    chunk, wo = u.shape[3], u.shape[4]
    vp = 4 * CHUNKS * chunk
    wi = picked_rows.shape[2]
    ratio = wi // wo
    half, quarter = vp // 2, vp // 4
    steps = layers * CHUNKS
    plane = 2 * vocab_count
    share = total // vocab_count
    me = core * vocab_count + voc
    at_end = jnp.logical_or(chip == 0, chip == chips - 1)
    holder = seq // ratio
    holds = holder == voc
    home = (voc * ratio) // 2
    at_home = chip == home

    def u_copy(k):
        return pltpu.make_async_copy(u_hbm.at[:, :, k], u.at[:, :, k], u_sem.at[k])

    def t_copy(l):
        return pltpu.make_async_copy(t_hbm.at[l], tr.at[l], t_sem.at[l])

    def remote(src, dst, send, recv, device):
        return pltpu.make_async_remote_copy(
            src_ref=src, dst_ref=dst, send_sem=send, recv_sem=recv, device_id=device, device_id_type=MESH
        )

    meta[...] = jnp.full(meta.shape, count[0], i32)
    meta[:, :cap] = wanted_ref[...]

    def settle(what, sem):
        return remote(what, what, sem, sem, partner)

    partner = (chip * 2 + 1 - core, voc)

    @pl.loop(0, layers - 1)
    def _(l):
        t_copy(l).start()

    @pl.loop(0, CHUNKS)
    def _(k):
        u_copy(k).start()

    barrier = pltpu.get_barrier_semaphore()

    def in_plane(p):
        q = lax.rem(me + p, plane)
        return q, (chip * 2 + q // vocab_count, lax.rem(q, vocab_count))

    def in_line(p):
        q = lax.rem(chip + p, chips)
        return q, (q * 2 + core, voc)

    def in_column(p):
        q = lax.rem(seq + p, seq_count)
        return q, (q, voc)

    def in_group(p):
        q = lax.rem(voc + p, vocab_count)
        return q, (seq, q)

    @pl.loop(1, plane)
    def _(p):
        pl.semaphore_signal(barrier, inc=1, device_id=in_plane(p)[1], device_id_type=MESH)

    @pl.loop(1, seq_count)
    def _(p):
        pl.semaphore_signal(barrier, inc=1, device_id=in_column(p)[1], device_id_type=MESH)

    with jax.named_scope('barrier'):
        pl.semaphore_wait(barrier, plane - 1 + seq_count - 1)

    def meta_copy(p, slot):
        return remote(meta, meta_recv.at[slot], msend_sem.at[0], mrecv_sem.at[0], in_column(p)[1])

    @pl.loop(1, seq_count)
    def _(p):
        meta_copy(p, seq).start()

    meta_recv[seq] = meta[...]

    def block(s):
        return pl.ds(pl.multiple_of(s * cap, cap), cap)

    def row_src(i):
        return picked_rows.at[i]

    def row_copy(i, source, d, src=None):
        to = jnp.minimum(chip + 1, chips - 1) if d == 0 else jnp.maximum(chip - 1, 0)
        here = rows.at[i, block(source * 2 + core)]
        return remote(
            here if src is None else src, here, rsend_sem.at[i, d], rrecv_sem.at[i, source], (to * 2 + core, voc)
        )

    def passes(d):
        return chip < chips - 1 if d == 0 else chip > 0

    def home_copy(source):
        here = rows.at[0, block(source * 2 + core)]
        return remote(picked_rows.at[0], here, rsend_sem.at[0, 0], rrecv_sem.at[0, source], (home * 2 + core, voc))

    def forward_copy(i, source, src=None):
        part = rows.at[i, block(source * 2 + core)]
        return remote(part if src is None else src, part, fsend_sem.at[i], frecv_sem.at[i], partner)

    def depart(i):
        for d in range(2):
            @pl.when(passes(d))
            def _():
                row_copy(i, chip, d, row_src(i)).start()

        forward_copy(i, chip, row_src(i)).start()

    @pl.when(at_home)
    def _():
        forward_copy(0, chip, picked_rows.at[0]).start()

    @pl.when(jnp.logical_not(at_home))
    def _():
        home_copy(chip).start()

    for i in range(layers):
        rows[i, block(seq), :] = row_src(i)[...]

    @pl.when(jnp.logical_not(at_home))
    def _():
        home_copy(chip).wait_send()

    depart(1)
    acc[...] = jnp.zeros_like(acc)

    def places():
        settle(meta_recv.at[pl.ds(0, seq_count - 1)], mrecv_sem.at[0]).wait_recv()
        every = jnp.concatenate([meta_recv[q] for q in range(seq_count)], axis=0)
        slots = seq_count * cap
        lane = lax.broadcasted_iota(i32, (1, slots), 1)
        owner = lax.broadcasted_iota(i32, (seq_count, slots), 1) // cap
        row = lax.broadcasted_iota(i32, (seq_count, slots), 0)
        counted = jnp.broadcast_to(every[:, cap : cap + 1], (seq_count, slots))
        counts = jnp.sum(jnp.where(row == owner, counted, 0), axis=0, keepdims=True)
        starts = jnp.sum(jnp.where(row < owner, counted, 0), axis=0, keepdims=True)
        wide = every.shape[1]
        spread = (
            lax.broadcasted_iota(i32, (wide, slots), 0) == lax.broadcasted_iota(i32, (wide, slots), 1) % cap
        ).astype(f32).astype(bf16)
        high = every // 256
        low = every - high * 256

        def lanes(byte):
            laid = jnp.dot(byte.astype(f32).astype(bf16), spread, preferred_element_type=f32)
            return jnp.sum(jnp.where(row == owner, laid, 0.0), axis=0, keepdims=True)

        slot = lane % cap
        place = jnp.where(slot < counts, starts + slot, -1)
        match = (lax.broadcasted_iota(i32, (total, slots), 0) == place).astype(f32).astype(bf16)
        hit[...] = match
        table = jnp.concatenate(
            [lanes(high), lanes(low), (place + 1).astype(f32), jnp.zeros((5, slots), f32)], axis=0
        ).astype(bf16)
        names = lax.dot_general(table, match, (((1,), (1,)), ((), ())), preferred_element_type=f32)
        tgt[...] = (names[0:1] * 256.0 + names[1:2]).astype(i32)
        mine = (
            lax.broadcasted_iota(i32, (cap, slots), 0) + seq * cap == lax.broadcasted_iota(i32, (cap, slots), 1)
        ).astype(f32).astype(bf16)
        spots = lax.dot_general(mine, table, (((1,), (1,)), ((), ())), preferred_element_type=f32)
        spot_col[...] = jnp.broadcast_to(spots[:, 2:3] - 1.0, spot_col.shape)

    def wants(i, then):
        pl.when(jnp.logical_or(i > 0, at_home))(then)

    def gather_home():
        @pl.loop(1, chips)
        def _(p):
            q, _ = in_line(p)
            home_copy(q).wait_recv()
            forward_copy(0, q).start()

    def relay(i):
        @pl.loop(1, chips)
        def _(p):
            for d in range(2):
                source = chip - p if d == 0 else chip + p

                @pl.when(source >= 0 if d == 0 else source < chips)
                def _():
                    row_copy(i, source, d).wait_recv()

                    @pl.when(passes(d))
                    def _():
                        row_copy(i, source, d).start()

                    forward_copy(i, source).start()

    def early(i):
        pl.when(jnp.logical_and(i == 0, at_home))(gather_home)

        @pl.when(jnp.logical_and(i > 0, jnp.logical_not(at_end)))
        def _():
            relay(i)

        for later in range(2, layers):
            pl.when(i == later - 2)(lambda: depart(later))

    def late(i):
        @pl.when(jnp.logical_and(i > 0, at_end))
        def _():
            relay(i)

    def part_of(q):
        return pl.ds(pl.multiple_of(q * share, share), share)

    def group_copy(i, p, slot):
        q, there = in_group(p)
        return remote(
            rs_src.at[i, part_of(q)], rs_recv.at[i, slot], gsend_sem.at[i], grecv_sem.at[i], there
        )

    def translate(i):
        def go():
            settle(rows.at[i, pl.ds(0, chips * cap)], frecv_sem.at[i]).wait_recv()

            packed[...] = jnp.dot(hit[...], rows[i], preferred_element_type=f32).astype(bf16)

            @pl.when(i > 0)
            def _():
                t_copy(i - 1).wait()
                part[...] = jnp.dot(packed[...], tr[i - 1], preferred_element_type=f32)

            @pl.when(holds)
            def _():
                start = pl.multiple_of(lax.rem(seq, ratio) * wo, wo)
                kept = packed[:, pl.ds(start, wo)].astype(f32)

                @pl.when(i > 0)
                def _():
                    part[...] = part[...] + kept

                @pl.when(i == 0)
                def _():
                    part[...] = kept

            @pl.when(jnp.logical_or(i > 0, holds))
            def _():
                rs_src[i] = xcode.enc(part[...])

                @pl.loop(1, vocab_count)
                def _(p):
                    group_copy(i, p, voc).start()

                rs_own[i] = part[part_of(voc), :]

        wants(i, go)

    def y_copy(i, p, owner):
        return remote(
            y.at[i, part_of(owner)], y.at[i, part_of(owner)], ysend_sem.at[i], yrecv_sem.at[i],
            in_group(p)[1],
        )

    def sq_copy(i, p, owner):
        return remote(
            sq_part.at[i, owner], sq_part.at[i, owner], qsend_sem.at[i], qrecv_sem.at[i], in_group(p)[1]
        )

    def scale(i):
        def go(x):
            y[i, part_of(voc), :] = (x * gain[...].reshape(1, wo)).astype(bf16)
            column = jnp.sum(x * x, axis=1, keepdims=True)
            lane = lax.broadcasted_iota(i32, (share, total), 1)
            row = lax.broadcasted_iota(i32, (share, total), 0) + voc * share
            sq_part[i, voc] = jnp.sum(jnp.where(lane == row, column, 0.0), axis=0, keepdims=True)

            @pl.loop(1, vocab_count)
            def _(p):
                y_copy(i, p, voc).start()

            @pl.loop(1, vocab_count)
            def _(p):
                sq_copy(i, p, voc).start()

        @pl.when(i > 0)
        def _():
            settle(rs_recv.at[i, pl.ds(0, vocab_count - 1)], grecv_sem.at[i]).wait_recv()
            x = rs_own[i] + bias[pl.ds(i - 1, 1), :]
            for p in range(1, vocab_count):
                q, _ = in_group(p)
                x = x + xcode.dec(rs_recv[i, q])
            go(x)

        @pl.when(jnp.logical_and(i == 0, holds))
        def _():
            go(rs_own[0])

        @pl.when(jnp.logical_and(i == 0, jnp.logical_not(holds)))
        def _():
            settle(rs_recv.at[0, 0], grecv_sem.at[0]).wait_recv()
            go(xcode.dec(rs_recv[0, holder]))

    def end_device(e):
        return jnp.where(e < 2, 0, seq_count - 2) + lax.rem(e, 2)

    def v_copy(i, e, source):
        return remote(
            sq_src.at[i], sq_recv.at[i, source], vsend_sem.at[i], vrecv_sem.at[i], (end_device(e), voc)
        )

    def collect(i):
        settle(y.at[i, pl.ds(0, (vocab_count - 1) * share)], yrecv_sem.at[i]).wait_recv()
        settle(sq_part.at[i, pl.ds(0, vocab_count - 1)], qrecv_sem.at[i]).wait_recv()

        sums = sq_part[i, 0]
        for q in range(1, vocab_count):
            sums = sums + sq_part[i, q]
        sq_src[i] = sums

        @pl.loop(0, 4)
        def _(e):
            @pl.when(end_device(e) != seq)
            def _():
                v_copy(i, e, seq).start()

        @pl.when(at_end)
        def _():
            sq_recv[i, seq] = sums

    def pair_copy(t):
        return remote(
            psend.at[lax.rem(t, SLOTS)], precv.at[t], psend_sem.at[lax.rem(t, SLOTS)], precv_sem.at[t], partner
        )

    def line_copy(k, d):
        to = jnp.minimum(chip + 1, chips - 1) if d == 0 else jnp.maximum(chip - 1, 0)
        return remote(
            zsend.at[d, k], zrecv.at[k, d], zsend_sem.at[d], zrecv_sem.at[k, d], (to * 2 + core, voc)
        )

    def product(owner, d, j, yl):
        return lax.dot_general(u[owner, d, j], yl, (((1,), (1,)), ((), ())), preferred_element_type=f32)

    def fold(value):
        return jnp.sum(value.reshape(chunk // 8, 8, total), axis=0)

    def finish(k, d, value):
        i, j = k // CHUNKS, lax.rem(k, CHUNKS)

        @pl.when(j == 0)
        def _():
            settle(sq_recv.at[i, pl.ds(0, seq_count - 1)], vrecv_sem.at[i]).wait_recv()

            squares = sq_recv[i, 0]
            for q in range(1, seq_count):
                squares = squares + sq_recv[i, q]
            fac[i] = lax.rsqrt(squares * (1.0 / model) + 1e-05)

        logit = value * fac[i]
        base = voc * vp + core * half + d * quarter + j * chunk
        spot = lax.broadcasted_iota(i32, (chunk, total), 0) + base
        grown = jnp.exp(logit)
        acc[i] += fold(grown)
        acc[layers + i] += fold(jnp.where(spot == tgt[...], logit, 0.0))

        @pl.when(i == 0)
        def _():
            z3[j] = logit
            e3[j] = grown

        @pl.when(i > 0)
        def _():
            acc[2 * layers + i] += fold(e3[j] * (z3[j] - logit))

    def forward(k, d):
        first = chip == (0 if d == 0 else chips - 1)
        last = chip == (chips - 1 if d == 0 else 0)

        @pl.when(jnp.logical_not(first))
        def _():
            with jax.named_scope('linewait'):
                line_copy(k, d).wait_recv()
            own[k, d] = own[k, d] + code.dec(zrecv[k, d])

        @pl.when(jnp.logical_not(last))
        def _():
            zsend[d, k] = code.enc(own[k, d])
            line_copy(k, d).start()

        @pl.when(last)
        def _():
            finish(k, d, own[k, d])

    def stage(t, turn, ahead, then):
        i = t // CHUNKS + ahead

        @pl.when(jnp.logical_and(lax.rem(t, CHUNKS) == turn, jnp.logical_and(i >= 0, i < layers)))
        def _():
            with jax.named_scope(then.__name__):
                then(i)

    turns = [(CHUNKS * k) // 4 for k in range(4)]

    @pl.loop(LEAD - 2 * CHUNKS - (CHUNKS - turns[3]), LEAD + steps + 1 + LAG * (chips - 1))
    def _(now):
        t = now - LEAD
        stage(now, turns[0], -LEAD // CHUNKS, collect)
        stage(now, turns[3], 3 - LEAD // CHUNKS, early)
        pl.when(t == turns[3] - 3 * CHUNKS)(places)
        stage(now, turns[1], 1 - LEAD // CHUNKS, scale)
        stage(now, turns[2], 2 - LEAD // CHUNKS, late)
        stage(now, turns[2], 2 - LEAD // CHUNKS, translate)

        @pl.when(jnp.logical_and(t >= 0, t < CHUNKS))
        def _():
            u_copy(t).wait()

        @pl.when(jnp.logical_and(t >= 0, t < steps))
        def _():
            i, j = t // CHUNKS, lax.rem(t, CHUNKS)
            yl = y[i]
            scope = jax.named_scope('dots'); scope.__enter__()

            @pl.when(t >= SLOTS)
            def _():
                pair_copy(t - SLOTS).wait_send()

            for d in range(2):
                psend[lax.rem(t, SLOTS), d] = product(1 - core, d, j, yl)
            pair_copy(t).start()
            for d in range(2):
                own[t, d] = product(core, d, j, yl)
            scope.__exit__(None, None, None)

        @pl.when(jnp.logical_and(t >= 1, t <= steps))
        def _():
            with jax.named_scope('pairsum'):
                pair_copy(t - 1).wait_recv()
                own[t - 1] = own[t - 1] + precv[t - 1]

        for d in range(2):
            k = t - 1 - LAG * (chip if d == 0 else chips - 1 - chip)

            @pl.when(jnp.logical_and(k >= 0, k < steps))
            def _():
                with jax.named_scope('fwd%d' % d):
                    forward(k, d)

    def stat_copy(p, slot):
        return remote(stat_send, stat_recv.at[slot], ssend_sem.at[0], srecv_sem.at[0], in_plane(p)[1])

    end = jnp.where(chip == 0, 0, 1)

    def line_stat(p, side):
        return remote(line_send, line_recv.at[side], lsend_sem.at[0], lrecv_sem.at[side], in_line(p)[1])

    @pl.when(at_end)
    def _():
        stat = jnp.concatenate(
            [jnp.sum(acc[i], axis=0, keepdims=True) for i in range(3 * layers)]
            + [jnp.zeros((stat_send.shape[0] - 3 * layers, total), f32)] * (stat_send.shape[0] > 3 * layers),
            axis=0,
        )
        stat_send[...] = stat
        stat_recv[me] = stat

        @pl.loop(1, plane)
        def _(p):
            stat_copy(p, me).start()

        with jax.named_scope('planewait'):
            settle(stat_recv.at[pl.ds(0, plane - 1)], srecv_sem.at[0]).wait_recv()

        full = stat_recv[0]
        for q in range(1, plane):
            full = full + stat_recv[q]
        line_send[...] = full
        line_recv[end] = full

        @pl.loop(1, chips)
        def _(p):
            line_stat(p, end).start()

    settle(meta_recv.at[pl.ds(0, seq_count - 1)], msend_sem.at[0]).wait_send()

    @pl.loop(0, layers)
    def _(i):
        for c in range(chips):
            for d in range(2):
                count_d = c + 1 if d == 0 else chips - c
                if (c < chips - 1) if d == 0 else (c > 0):
                    @pl.when(jnp.logical_and(i > 0, chip == c))
                    def _():
                        settle(rows.at[i, pl.ds(0, count_d * cap)], rsend_sem.at[i, d]).wait_send()

        @pl.when(jnp.logical_or(i > 0, at_home))
        def _():
            settle(rows.at[i, pl.ds(0, chips * cap)], fsend_sem.at[i]).wait_send()

        @pl.when(jnp.logical_or(i > 0, holds))
        def _():
            settle(rs_recv.at[i, pl.ds(0, vocab_count - 1)], gsend_sem.at[i]).wait_send()

        settle(y.at[i, pl.ds(0, (vocab_count - 1) * share)], ysend_sem.at[i]).wait_send()
        settle(sq_part.at[i, pl.ds(0, vocab_count - 1)], qsend_sem.at[i]).wait_send()

        @pl.when(at_end)
        def _():
            settle(sq_recv.at[i, pl.ds(0, 3)], vsend_sem.at[i]).wait_send()

        @pl.when(jnp.logical_not(at_end))
        def _():
            settle(sq_recv.at[i, pl.ds(0, 4)], vsend_sem.at[i]).wait_send()

    @pl.loop(steps - SLOTS, steps)
    def _(t):
        pair_copy(t).wait_send()

    for d in range(2):
        @pl.when(chip != (chips - 1 if d == 0 else 0))
        def _():
            settle(zsend.at[d], zsend_sem.at[d]).wait_send()

    @pl.when(at_end)
    def _():
        settle(stat_recv.at[pl.ds(0, plane - 1)], ssend_sem.at[0]).wait_send()
        settle(stat_recv.at[pl.ds(0, chips - 1)], lsend_sem.at[0]).wait_send()

    for side in range(2):
        @pl.when(chip != (0 if side == 0 else chips - 1))
        def _():
            with jax.named_scope('statwait'):
                line_stat(1, side).wait_recv()

    scope2 = jax.named_scope('final'); scope2.__enter__()
    full = line_recv[0] + line_recv[1]
    total_exp, picked = full[:layers], full[layers : 2 * layers]
    cross = full[2 * layers + 1 : 3 * layers]
    log_total = jnp.log(total_exp)
    result = [picked[l : l + 1] - log_total[l : l + 1] for l in list(range(1, layers)) + [0]]
    for l in range(1, layers):
        result.append(cross[l - 1 : l] / total_exp[0:1] - log_total[0:1] + log_total[l : l + 1])
    lane = lax.broadcasted_iota(i32, (cap, total), 1).astype(f32)
    owned = lane == spot_col[...]
    place = lax.broadcasted_iota(i32, (cap, 128), 1)
    out = jnp.zeros((cap, 128), f32)
    for l, value in enumerate(result):
        column = jnp.sum(jnp.where(owned, value, 0.0), axis=1, keepdims=True)
        out = jnp.where(place == l, column, out)
    turned = out.T
    for l in range(layers):
        prob_ref[l] = turned[l : l + 1]
    for l in range(layers - 1):
        kl_ref[l] = turned[layers + l : layers + l + 1]
    scope2.__exit__(None, None, None)

def pick_kernel(layers, cap, picks, probe_hbm, final_hbm, out_ref, found, sem):
    @pl.loop(0, cap)
    def _(k):
        first = pl.ds(pl.multiple_of(picks[0, k] // PACK * PACK, PACK), PACK)
        spot = pl.ds(pl.multiple_of(k * PACK, PACK), PACK)
        pltpu.make_async_copy(final_hbm.at[first], found.at[0, spot], sem.at[0]).start()
        for l in range(1, layers):
            pltpu.make_async_copy(probe_hbm.at[l - 1, first], found.at[l, spot], sem.at[l]).start()

    row = lax.broadcasted_iota(i32, (cap, cap * PACK), 0)
    wants = jnp.zeros((cap, cap * PACK), i32)
    for k in range(cap):
        wants = jnp.where(row == k, k * PACK + picks[0, k] % PACK, wants)
    match = (lax.broadcasted_iota(i32, (cap, cap * PACK), 1) == wants).astype(f32).astype(bf16)
    for l in range(layers):
        pltpu.make_async_copy(found.at[l], found.at[l], sem.at[l]).wait()
        out_ref[l] = jnp.dot(match, found[l], preferred_element_type=f32).astype(bf16)

def pick(answer_rows, probe_states, final_states):
    layers, cap, wi = probe_states.shape[0] + 1, answer_rows.shape[1], final_states.shape[1]
    hbm = pl.BlockSpec(memory_space=pl.ANY)
    return pl.pallas_call(
        lambda *refs: pick_kernel(layers, cap, *refs),
        out_shape=jax.ShapeDtypeStruct((layers, cap, wi), bf16),
        in_specs=[pl.BlockSpec(memory_space=pltpu.SMEM), hbm, hbm],
        out_specs=pl.BlockSpec(memory_space=pltpu.VMEM),
        scratch_shapes=[pltpu.VMEM((layers, cap * PACK, wi), bf16), pltpu.SemaphoreType.DMA((layers,))],
        name="pick",
    )(answer_rows, probe_states, final_states)

def readout(rows, count, wanted, bias, gain, translator, unembed, seq_count, vocab_count, total, model):
    layers, cap, wi = rows.shape
    vp, wo = unembed.shape
    steps = layers * CHUNKS
    chunk = vp // 4 // CHUNKS
    plane, chips = 2 * vocab_count, seq_count // 2
    share = total // vocab_count
    code = Code(GAIN_MAX * UNEMBED_MAX * model * (STATE_MAX + BIAS_MAX + model * STATE_MAX * MATRIX_MAX))
    xcode = Code(STATE_MAX + BIAS_MAX + model * STATE_MAX * MATRIX_MAX)
    deep = -(-3 * layers // 8) * 8
    dma = pltpu.SemaphoreType.DMA
    vmem = pl.BlockSpec(memory_space=pltpu.VMEM)
    hbm = pl.BlockSpec(memory_space=pl.ANY)
    body = lambda *refs: kernel(layers, total, cap, seq_count, vocab_count, model, code, xcode, *refs)
    return pl.pallas_call(
        body,
        out_shape=(
            jax.ShapeDtypeStruct((layers, 1, cap), f32),
            jax.ShapeDtypeStruct((layers - 1, 1, cap), f32),
        ),
        in_specs=[vmem, pl.BlockSpec(memory_space=pltpu.SMEM), vmem, vmem, vmem, hbm, hbm],
        out_specs=(vmem, vmem),
        scratch_shapes=[
            pltpu.VMEM((2, 2, CHUNKS, chunk, wo), bf16),
            pltpu.VMEM((layers - 1, wi, wo), bf16),
            pltpu.VMEM((1, 128), i32),
            pltpu.VMEM((layers, seq_count * cap, wi), bf16),
            pltpu.VMEM((total, wi), bf16),
            pltpu.VMEM((total, seq_count * cap), bf16),
            pltpu.VMEM((1, total), i32),
            pltpu.VMEM((cap, total), f32),
            pltpu.VMEM((seq_count, 1, 128), i32),
            pltpu.VMEM((total, wo), f32),
            pltpu.VMEM((layers, share, wo), f32),
            pltpu.VMEM((layers, total, wo), i16),
            pltpu.VMEM((layers, vocab_count, share, wo), i16),
            pltpu.VMEM((layers, total, wo), bf16),
            pltpu.VMEM((layers, vocab_count, 1, total), f32),
            pltpu.VMEM((layers, 1, total), f32),
            pltpu.VMEM((layers, seq_count, 1, total), f32),
            pltpu.VMEM((layers, 1, total), f32),
            pltpu.VMEM((steps, 2, chunk, total), f32),
            pltpu.VMEM((SLOTS, 2, chunk, total), f32),
            pltpu.VMEM((steps, 2, chunk, total), f32),
            pltpu.VMEM((2, steps, chunk, total), i16),
            pltpu.VMEM((steps, 2, chunk, total), i16),
            pltpu.VMEM((CHUNKS, chunk, total), f32),
            pltpu.VMEM((CHUNKS, chunk, total), f32),
            pltpu.VMEM((3 * layers, 8, total), f32),
            pltpu.VMEM((deep, total), f32),
            pltpu.VMEM((plane, deep, total), f32),
            pltpu.VMEM((deep, total), f32),
            pltpu.VMEM((2, deep, total), f32),
            dma((CHUNKS,)),
            dma((layers - 1,)),
            dma((1,)),
            dma((1,)),
            dma((layers, 2)),
            dma((layers, chips)),
            dma((layers,)),
            dma((layers,)),
            dma((layers,)),
            dma((layers,)),
            dma((layers,)),
            dma((layers,)),
            dma((layers,)),
            dma((layers,)),
            dma((layers,)),
            dma((layers,)),
            dma((SLOTS,)),
            dma((steps,)),
            dma((2,)),
            dma((steps, 2)),
            dma((1,)),
            dma((1,)),
            dma((1,)),
            dma((2,)),
        ],
        compiler_params=pltpu.CompilerParams(
            collective_id=0, has_side_effects=True, vmem_limit_bytes=63 << 20
        ),
        name="readout",
    )(rows, count, wanted, bias, gain, translator, unembed.reshape(2, 2, CHUNKS, chunk, wo))

def body(
    probe_states,
    final_states,
    translator,
    translator_bias,
    norm_gain,
    unembed,
    answer_rows,
    answer_count,
    targets,
):
    seq_count = lax.axis_size("seq")
    vocab_count = lax.axis_size("vocab")
    model = probe_states.shape[2] * vocab_count
    return readout(
        pick(answer_rows, probe_states, final_states),
        answer_count,
        targets,
        translator_bias,
        norm_gain,
        translator,
        unembed,
        seq_count,
        vocab_count,
        seq_count * FLAG_DEV,
        model,
    )

def solution(mesh):
    in_specs = (
        P(None, "seq", "vocab"),
        P("seq", "vocab"),
        P(None, "vocab", "seq"),
        P(None, "seq"),
        P("seq"),
        P("vocab", "seq"),
        P("seq", None),
        P("seq"),
        P("seq", None),
    )
    out_specs = (P(None, "seq", None), P(None, "seq", None))
    return jax.shard_map(body, mesh=mesh, in_specs=in_specs, out_specs=out_specs, check_vma=False)
```

```python
import math
import jax
import jax.numpy as jnp
from jax import lax
from jax.experimental import pallas as pl
from jax.experimental.pallas import tpu as pltpu
from jax.sharding import PartitionSpec as P

FLAG_DEV = 16
STATE_MAX, MATRIX_MAX, BIAS_MAX, GAIN_MAX, UNEMBED_MAX = 6.0, 0.078125, 4.0, 1.5, 0.21875
CHUNKS = 4
LAG = 2
SLOTS = 4
PACK = 8
LEAD = 3 * CHUNKS
MESH = pl.DeviceIdType.MESH
f32, bf16, i16, i32 = jnp.float32, jnp.bfloat16, jnp.int16, jnp.int32

class Code:
    def __init__(self, widest):
        self.knee = 7.5e-4
        self.scale = 32700.0 / math.log2(1.0 + 1.02 * widest / self.knee)

    def enc(self, value):
        level = jnp.log2(1.0 + jnp.abs(value) * (1.0 / self.knee)) * self.scale
        return jnp.round(jnp.where(value < 0, -level, level)).astype(i32).astype(i16)

    def dec(self, code):
        level = code.astype(i32).astype(f32)
        size = (jnp.exp2(jnp.abs(level) * (1.0 / self.scale)) - 1.0) * self.knee
        return jnp.where(level < 0, -size, size)

def kernel(
    layers, total, cap, seq_count, vocab_count, model, code, xcode,
    picked_rows, count, wanted_ref, bias, gain, t_hbm, u_hbm, out_ref,
    u, tr, meta, rows, packed, hit, tgt, spot_col, meta_recv, part, rs_own, rs_src, rs_recv, y, sq_part, sq_src, sq_recv, fac,
    own, psend, precv, zsend, zrecv, z3, e3, acc, stat_send, stat_recv, line_send, line_recv,
    u_sem, t_sem, msend_sem, mrecv_sem, rsend_sem, rrecv_sem, fsend_sem, frecv_sem, gsend_sem, grecv_sem,
    ysend_sem, yrecv_sem, qsend_sem, qrecv_sem, vsend_sem, vrecv_sem,
    psend_sem, precv_sem, zsend_sem, zrecv_sem, ssend_sem, srecv_sem, lsend_sem, lrecv_sem,
):
    seq, voc = lax.axis_index("seq"), lax.axis_index("vocab")
    chip, core = seq // 2, seq % 2
    chips = seq_count // 2
    chunk, wo = u.shape[3], u.shape[4]
    vp = 4 * CHUNKS * chunk
    wi = picked_rows.shape[2]
    ratio = wi // wo
    half, quarter = vp // 2, vp // 4
    steps = layers * CHUNKS
    plane = 2 * vocab_count
    share = total // vocab_count
    me = core * vocab_count + voc
    at_end = jnp.logical_or(chip == 0, chip == chips - 1)
    holder = seq // ratio
    holds = holder == voc
    home = (voc * ratio) // 2
    at_home = chip == home

    def u_copy(k):
        return pltpu.make_async_copy(u_hbm.at[:, :, k], u.at[:, :, k], u_sem.at[k])

    def t_copy(l):
        return pltpu.make_async_copy(t_hbm.at[l], tr.at[l], t_sem.at[l])

    def remote(src, dst, send, recv, device):
        return pltpu.make_async_remote_copy(
            src_ref=src, dst_ref=dst, send_sem=send, recv_sem=recv, device_id=device, device_id_type=MESH
        )

    barrier = pltpu.get_barrier_semaphore()

    def in_plane(p):
        q = lax.rem(me + p, plane)
        return q, (chip * 2 + q // vocab_count, lax.rem(q, vocab_count))

    def in_line(p):
        q = lax.rem(chip + p, chips)
        return q, (q * 2 + core, voc)

    def in_column(p):
        q = lax.rem(seq + p, seq_count)
        return q, (q, voc)

    def in_group(p):
        q = lax.rem(voc + p, vocab_count)
        return q, (seq, q)

    @pl.loop(1, plane)
    def _(p):
        pl.semaphore_signal(barrier, inc=1, device_id=in_plane(p)[1], device_id_type=MESH)

    @pl.loop(1, seq_count)
    def _(p):
        pl.semaphore_signal(barrier, inc=1, device_id=in_column(p)[1], device_id_type=MESH)

    meta[...] = jnp.full(meta.shape, count[0], i32)
    meta[:, :cap] = wanted_ref[...]

    def settle(what, sem):
        return remote(what, what, sem, sem, partner)

    partner = (chip * 2 + 1 - core, voc)

    @pl.loop(0, layers - 1)
    def _(l):
        t_copy(l).start()

    @pl.loop(0, CHUNKS)
    def _(k):
        u_copy(k).start()

    with jax.named_scope('barrier'):
        pl.semaphore_wait(barrier, plane - 1 + seq_count - 1)

    def meta_copy(p, slot):
        return remote(meta, meta_recv.at[slot], msend_sem.at[0], mrecv_sem.at[0], in_column(p)[1])

    @pl.loop(1, seq_count)
    def _(p):
        meta_copy(p, seq).start()

    meta_recv[seq] = meta[...]

    def block(s):
        return pl.ds(pl.multiple_of(s * cap, cap), cap)

    def row_src(i):
        return picked_rows.at[i]

    def row_copy(i, source, d, src=None):
        to = jnp.minimum(chip + 1, chips - 1) if d == 0 else jnp.maximum(chip - 1, 0)
        here = rows.at[i, block(source * 2 + core)]
        return remote(
            here if src is None else src, here, rsend_sem.at[i, d], rrecv_sem.at[i, source], (to * 2 + core, voc)
        )

    def passes(d):
        return chip < chips - 1 if d == 0 else chip > 0

    def home_copy(source):
        here = rows.at[0, block(source * 2 + core)]
        return remote(picked_rows.at[0], here, rsend_sem.at[0, 0], rrecv_sem.at[0, source], (home * 2 + core, voc))

    def forward_copy(i, source, src=None):
        part = rows.at[i, block(source * 2 + core)]
        return remote(part if src is None else src, part, fsend_sem.at[i], frecv_sem.at[i], partner)

    def depart(i):
        for d in range(2):
            @pl.when(passes(d))
            def _():
                row_copy(i, chip, d, row_src(i)).start()

        forward_copy(i, chip, row_src(i)).start()

    @pl.when(at_home)
    def _():
        forward_copy(0, chip, picked_rows.at[0]).start()

    @pl.when(jnp.logical_not(at_home))
    def _():
        home_copy(chip).start()

    for i in range(layers):
        rows[i, block(seq), :] = row_src(i)[...]

    @pl.when(jnp.logical_not(at_home))
    def _():
        home_copy(chip).wait_send()

    depart(1)
    acc[...] = jnp.zeros_like(acc)

    def places():
        settle(meta_recv.at[pl.ds(0, seq_count - 1)], mrecv_sem.at[0]).wait_recv()
        every = jnp.concatenate([meta_recv[q] for q in range(seq_count)], axis=0)
        slots = seq_count * cap
        lane = lax.broadcasted_iota(i32, (1, slots), 1)
        owner = lax.broadcasted_iota(i32, (seq_count, slots), 1) // cap
        row = lax.broadcasted_iota(i32, (seq_count, slots), 0)
        counted = jnp.broadcast_to(every[:, cap : cap + 1], (seq_count, slots))
        counts = jnp.sum(jnp.where(row == owner, counted, 0), axis=0, keepdims=True)
        starts = jnp.sum(jnp.where(row < owner, counted, 0), axis=0, keepdims=True)
        wide = every.shape[1]
        spread = (
            lax.broadcasted_iota(i32, (wide, slots), 0) == lax.broadcasted_iota(i32, (wide, slots), 1) % cap
        ).astype(f32).astype(bf16)
        high = every // 256
        low = every - high * 256

        def lanes(byte):
            laid = jnp.dot(byte.astype(f32).astype(bf16), spread, preferred_element_type=f32)
            return jnp.sum(jnp.where(row == owner, laid, 0.0), axis=0, keepdims=True)

        slot = lane % cap
        place = jnp.where(slot < counts, starts + slot, -1)
        match = (lax.broadcasted_iota(i32, (total, slots), 0) == place).astype(f32).astype(bf16)
        hit[...] = match
        table = jnp.concatenate(
            [lanes(high), lanes(low), (place + 1).astype(f32), jnp.zeros((5, slots), f32)], axis=0
        ).astype(bf16)
        names = lax.dot_general(table, match, (((1,), (1,)), ((), ())), preferred_element_type=f32)
        tgt[...] = (names[0:1] * 256.0 + names[1:2]).astype(i32)
        mine = (
            lax.broadcasted_iota(i32, (cap, slots), 0) + seq * cap == lax.broadcasted_iota(i32, (cap, slots), 1)
        ).astype(f32).astype(bf16)
        spots = lax.dot_general(mine, table, (((1,), (1,)), ((), ())), preferred_element_type=f32)
        spot_col[...] = jnp.broadcast_to(spots[:, 2:3] - 1.0, spot_col.shape)

    def wants(i, then):
        pl.when(jnp.logical_or(i > 0, at_home))(then)

    def gather_home():
        @pl.loop(1, chips)
        def _(p):
            q, _ = in_line(p)
            home_copy(q).wait_recv()
            forward_copy(0, q).start()

    def relay(i):
        @pl.loop(1, chips)
        def _(p):
            for d in range(2):
                source = chip - p if d == 0 else chip + p

                @pl.when(source >= 0 if d == 0 else source < chips)
                def _():
                    row_copy(i, source, d).wait_recv()

                    @pl.when(passes(d))
                    def _():
                        row_copy(i, source, d).start()

                    forward_copy(i, source).start()

    def early(i):
        pl.when(jnp.logical_and(i == 0, at_home))(gather_home)

        @pl.when(jnp.logical_and(i > 0, jnp.logical_not(at_end)))
        def _():
            relay(i)

        for later in range(2, layers):
            pl.when(i == later - 2)(lambda: depart(later))

    def late(i):
        @pl.when(jnp.logical_and(i > 0, at_end))
        def _():
            relay(i)

    def part_of(q):
        return pl.ds(pl.multiple_of(q * share, share), share)

    def group_copy(i, p, slot):
        q, there = in_group(p)
        return remote(
            rs_src.at[i, part_of(q)], rs_recv.at[i, slot], gsend_sem.at[i], grecv_sem.at[i], there
        )

    def translate(i):
        def go():
            settle(rows.at[i, pl.ds(0, chips * cap)], frecv_sem.at[i]).wait_recv()

            packed[...] = jnp.dot(hit[...], rows[i], preferred_element_type=f32).astype(bf16)

            @pl.when(i > 0)
            def _():
                t_copy(i - 1).wait()
                part[...] = jnp.dot(packed[...], tr[i - 1], preferred_element_type=f32)

            @pl.when(holds)
            def _():
                start = pl.multiple_of(lax.rem(seq, ratio) * wo, wo)
                kept = packed[:, pl.ds(start, wo)].astype(f32)

                @pl.when(i > 0)
                def _():
                    part[...] = part[...] + kept

                @pl.when(i == 0)
                def _():
                    part[...] = kept

            @pl.when(jnp.logical_or(i > 0, holds))
            def _():
                rs_src[i] = xcode.enc(part[...])

                @pl.loop(1, vocab_count)
                def _(p):
                    group_copy(i, p, voc).start()

                rs_own[i] = part[part_of(voc), :]

        wants(i, go)

    def y_copy(i, p, owner):
        return remote(
            y.at[i, part_of(owner)], y.at[i, part_of(owner)], ysend_sem.at[i], yrecv_sem.at[i],
            in_group(p)[1],
        )

    def sq_copy(i, p, owner):
        return remote(
            sq_part.at[i, owner], sq_part.at[i, owner], qsend_sem.at[i], qrecv_sem.at[i], in_group(p)[1]
        )

    def scale(i):
        def go(x):
            y[i, part_of(voc), :] = (x * gain[...].reshape(1, wo)).astype(bf16)
            column = jnp.sum(x * x, axis=1, keepdims=True)
            lane = lax.broadcasted_iota(i32, (share, total), 1)
            row = lax.broadcasted_iota(i32, (share, total), 0) + voc * share
            sq_part[i, voc] = jnp.sum(jnp.where(lane == row, column, 0.0), axis=0, keepdims=True)

            @pl.loop(1, vocab_count)
            def _(p):
                y_copy(i, p, voc).start()

            @pl.loop(1, vocab_count)
            def _(p):
                sq_copy(i, p, voc).start()

        @pl.when(i > 0)
        def _():
            settle(rs_recv.at[i, pl.ds(0, vocab_count - 1)], grecv_sem.at[i]).wait_recv()
            x = rs_own[i] + bias[pl.ds(i - 1, 1), :]
            for p in range(1, vocab_count):
                q, _ = in_group(p)
                x = x + xcode.dec(rs_recv[i, q])
            go(x)

        @pl.when(jnp.logical_and(i == 0, holds))
        def _():
            go(rs_own[0])

        @pl.when(jnp.logical_and(i == 0, jnp.logical_not(holds)))
        def _():
            settle(rs_recv.at[0, 0], grecv_sem.at[0]).wait_recv()
            go(xcode.dec(rs_recv[0, holder]))

    def end_device(e):
        return jnp.where(e < 2, 0, seq_count - 2) + lax.rem(e, 2)

    def v_copy(i, e, source):
        return remote(
            sq_src.at[i], sq_recv.at[i, source], vsend_sem.at[i], vrecv_sem.at[i], (end_device(e), voc)
        )

    def collect(i):
        settle(y.at[i, pl.ds(0, (vocab_count - 1) * share)], yrecv_sem.at[i]).wait_recv()
        settle(sq_part.at[i, pl.ds(0, vocab_count - 1)], qrecv_sem.at[i]).wait_recv()

        sums = sq_part[i, 0]
        for q in range(1, vocab_count):
            sums = sums + sq_part[i, q]
        sq_src[i] = sums

        @pl.loop(0, 4)
        def _(e):
            @pl.when(end_device(e) != seq)
            def _():
                v_copy(i, e, seq).start()

        @pl.when(at_end)
        def _():
            sq_recv[i, seq] = sums

    def pair_copy(t):
        return remote(
            psend.at[lax.rem(t, SLOTS)], precv.at[t], psend_sem.at[lax.rem(t, SLOTS)], precv_sem.at[t], partner
        )

    def line_copy(k, d):
        to = jnp.minimum(chip + 1, chips - 1) if d == 0 else jnp.maximum(chip - 1, 0)
        return remote(
            zsend.at[d, k], zrecv.at[k, d], zsend_sem.at[d], zrecv_sem.at[k, d], (to * 2 + core, voc)
        )

    def product(owner, d, j, yl):
        return lax.dot_general(u[owner, d, j], yl, (((1,), (1,)), ((), ())), preferred_element_type=f32)

    def fold(value):
        return jnp.sum(value.reshape(chunk // 8, 8, total), axis=0)

    def finish(k, d, value):
        i, j = k // CHUNKS, lax.rem(k, CHUNKS)

        @pl.when(j == 0)
        def _():
            settle(sq_recv.at[i, pl.ds(0, seq_count - 1)], vrecv_sem.at[i]).wait_recv()

            squares = sq_recv[i, 0]
            for q in range(1, seq_count):
                squares = squares + sq_recv[i, q]
            fac[i] = lax.rsqrt(squares * (1.0 / model) + 1e-05)

        logit = value * fac[i]
        base = voc * vp + core * half + d * quarter + j * chunk
        spot = lax.broadcasted_iota(i32, (chunk, total), 0) + base
        grown = jnp.exp(logit)
        acc[i] += fold(grown)
        acc[layers + i] += fold(jnp.where(spot == tgt[...], logit, 0.0))

        @pl.when(i == 0)
        def _():
            z3[j] = logit
            e3[j] = grown

        @pl.when(i > 0)
        def _():
            acc[2 * layers + i] += fold(e3[j] * (z3[j] - logit))

    def forward(k, d):
        first = chip == (0 if d == 0 else chips - 1)
        last = chip == (chips - 1 if d == 0 else 0)

        @pl.when(jnp.logical_not(first))
        def _():
            with jax.named_scope('linewait'):
                line_copy(k, d).wait_recv()
            own[k, d] = own[k, d] + code.dec(zrecv[k, d])

        @pl.when(jnp.logical_not(last))
        def _():
            zsend[d, k] = code.enc(own[k, d])
            line_copy(k, d).start()

        @pl.when(last)
        def _():
            finish(k, d, own[k, d])

    def stage(t, turn, ahead, then):
        i = t // CHUNKS + ahead

        @pl.when(jnp.logical_and(lax.rem(t, CHUNKS) == turn, jnp.logical_and(i >= 0, i < layers)))
        def _():
            with jax.named_scope(then.__name__):
                then(i)

    turns = [(CHUNKS * k) // 4 for k in range(4)]

    @pl.loop(LEAD - 2 * CHUNKS - (CHUNKS - turns[3]), LEAD + steps + 1 + LAG * (chips - 1))
    def _(now):
        t = now - LEAD
        stage(now, turns[0], -LEAD // CHUNKS, collect)
        stage(now, turns[3], 3 - LEAD // CHUNKS, early)
        pl.when(t == turns[3] - 3 * CHUNKS)(places)
        stage(now, turns[1], 1 - LEAD // CHUNKS, scale)
        stage(now, turns[2], 2 - LEAD // CHUNKS, late)
        stage(now, turns[2], 2 - LEAD // CHUNKS, translate)

        @pl.when(jnp.logical_and(t >= 0, t < CHUNKS))
        def _():
            u_copy(t).wait()

        @pl.when(jnp.logical_and(t >= 0, t < steps))
        def _():
            i, j = t // CHUNKS, lax.rem(t, CHUNKS)
            yl = y[i]
            scope = jax.named_scope('dots'); scope.__enter__()

            @pl.when(t >= SLOTS)
            def _():
                pair_copy(t - SLOTS).wait_send()

            for d in range(2):
                psend[lax.rem(t, SLOTS), d] = product(1 - core, d, j, yl)
            pair_copy(t).start()
            for d in range(2):
                own[t, d] = product(core, d, j, yl)
            scope.__exit__(None, None, None)

        @pl.when(jnp.logical_and(t >= 1, t <= steps))
        def _():
            with jax.named_scope('pairsum'):
                pair_copy(t - 1).wait_recv()
                own[t - 1] = own[t - 1] + precv[t - 1]

        for d in range(2):
            k = t - 1 - LAG * (chip if d == 0 else chips - 1 - chip)

            @pl.when(jnp.logical_and(k >= 0, k < steps))
            def _():
                with jax.named_scope('fwd%d' % d):
                    forward(k, d)

    def stat_copy(p, slot):
        return remote(stat_send, stat_recv.at[slot], ssend_sem.at[0], srecv_sem.at[0], in_plane(p)[1])

    end = jnp.where(chip == 0, 0, 1)

    def line_stat(p, side):
        return remote(line_send, line_recv.at[side], lsend_sem.at[0], lrecv_sem.at[side], in_line(p)[1])

    @pl.when(at_end)
    def _():
        stat = jnp.concatenate(
            [jnp.sum(acc[i], axis=0, keepdims=True) for i in range(3 * layers)]
            + [jnp.zeros((stat_send.shape[0] - 3 * layers, total), f32)] * (stat_send.shape[0] > 3 * layers),
            axis=0,
        )
        stat_send[...] = stat
        stat_recv[me] = stat

        @pl.loop(1, plane)
        def _(p):
            stat_copy(p, me).start()

        with jax.named_scope('planewait'):
            settle(stat_recv.at[pl.ds(0, plane - 1)], srecv_sem.at[0]).wait_recv()

        full = stat_recv[0]
        for q in range(1, plane):
            full = full + stat_recv[q]
        line_send[...] = full
        line_recv[end] = full

        @pl.loop(1, chips)
        def _(p):
            line_stat(p, end).start()

    settle(meta_recv.at[pl.ds(0, seq_count - 1)], msend_sem.at[0]).wait_send()

    @pl.loop(0, layers)
    def _(i):
        for c in range(chips):
            for d in range(2):
                count_d = c + 1 if d == 0 else chips - c
                if (c < chips - 1) if d == 0 else (c > 0):
                    @pl.when(jnp.logical_and(i > 0, chip == c))
                    def _():
                        settle(rows.at[i, pl.ds(0, count_d * cap)], rsend_sem.at[i, d]).wait_send()

        @pl.when(jnp.logical_or(i > 0, at_home))
        def _():
            settle(rows.at[i, pl.ds(0, chips * cap)], fsend_sem.at[i]).wait_send()

        @pl.when(jnp.logical_or(i > 0, holds))
        def _():
            settle(rs_recv.at[i, pl.ds(0, vocab_count - 1)], gsend_sem.at[i]).wait_send()

        settle(y.at[i, pl.ds(0, (vocab_count - 1) * share)], ysend_sem.at[i]).wait_send()
        settle(sq_part.at[i, pl.ds(0, vocab_count - 1)], qsend_sem.at[i]).wait_send()

        @pl.when(at_end)
        def _():
            settle(sq_recv.at[i, pl.ds(0, 3)], vsend_sem.at[i]).wait_send()

        @pl.when(jnp.logical_not(at_end))
        def _():
            settle(sq_recv.at[i, pl.ds(0, 4)], vsend_sem.at[i]).wait_send()

    @pl.loop(steps - SLOTS, steps)
    def _(t):
        pair_copy(t).wait_send()

    for d in range(2):
        @pl.when(chip != (chips - 1 if d == 0 else 0))
        def _():
            settle(zsend.at[d], zsend_sem.at[d]).wait_send()

    @pl.when(at_end)
    def _():
        settle(stat_recv.at[pl.ds(0, plane - 1)], ssend_sem.at[0]).wait_send()
        settle(stat_recv.at[pl.ds(0, chips - 1)], lsend_sem.at[0]).wait_send()

    for side in range(2):
        @pl.when(chip != (0 if side == 0 else chips - 1))
        def _():
            with jax.named_scope('statwait'):
                line_stat(1, side).wait_recv()

    scope2 = jax.named_scope('final'); scope2.__enter__()
    full = line_recv[0] + line_recv[1]
    total_exp, picked = full[:layers], full[layers : 2 * layers]
    cross = full[2 * layers + 1 : 3 * layers]
    log_total = jnp.log(total_exp)
    result = [picked[l : l + 1] - log_total[l : l + 1] for l in list(range(1, layers)) + [0]]
    for l in range(1, layers):
        result.append(cross[l - 1 : l] / total_exp[0:1] - log_total[0:1] + log_total[l : l + 1])
    lane = lax.broadcasted_iota(i32, (cap, total), 1).astype(f32)
    owned = lane == spot_col[...]
    place = lax.broadcasted_iota(i32, (cap, 128), 1)
    out = jnp.zeros((cap, 128), f32)
    for l, value in enumerate(result):
        column = jnp.sum(jnp.where(owned, value, 0.0), axis=1, keepdims=True)
        out = jnp.where(place == l, column, out)
    out_ref[...] = out
    scope2.__exit__(None, None, None)

def pick_kernel(layers, cap, picks, probe_hbm, final_hbm, out_ref, found, sem):
    @pl.loop(0, cap)
    def _(k):
        first = pl.ds(pl.multiple_of(picks[0, k] // PACK * PACK, PACK), PACK)
        spot = pl.ds(pl.multiple_of(k * PACK, PACK), PACK)
        pltpu.make_async_copy(final_hbm.at[first], found.at[0, spot], sem.at[0]).start()
        for l in range(1, layers):
            pltpu.make_async_copy(probe_hbm.at[l - 1, first], found.at[l, spot], sem.at[l]).start()

    row = lax.broadcasted_iota(i32, (cap, cap * PACK), 0)
    wants = jnp.zeros((cap, cap * PACK), i32)
    for k in range(cap):
        wants = jnp.where(row == k, k * PACK + picks[0, k] % PACK, wants)
    match = (lax.broadcasted_iota(i32, (cap, cap * PACK), 1) == wants).astype(f32).astype(bf16)
    for l in range(layers):
        pltpu.make_async_copy(found.at[l], found.at[l], sem.at[l]).wait()
        out_ref[l] = jnp.dot(match, found[l], preferred_element_type=f32).astype(bf16)

def pick(answer_rows, probe_states, final_states):
    layers, cap, wi = probe_states.shape[0] + 1, answer_rows.shape[1], final_states.shape[1]
    hbm = pl.BlockSpec(memory_space=pl.ANY)
    return pl.pallas_call(
        lambda *refs: pick_kernel(layers, cap, *refs),
        out_shape=jax.ShapeDtypeStruct((layers, cap, wi), bf16),
        in_specs=[pl.BlockSpec(memory_space=pltpu.SMEM), hbm, hbm],
        out_specs=pl.BlockSpec(memory_space=pltpu.VMEM),
        scratch_shapes=[pltpu.VMEM((layers, cap * PACK, wi), bf16), pltpu.SemaphoreType.DMA((layers,))],
        name="pick",
    )(answer_rows, probe_states, final_states)

def readout(rows, count, wanted, bias, gain, translator, unembed, seq_count, vocab_count, total, model):
    layers, cap, wi = rows.shape
    vp, wo = unembed.shape
    steps = layers * CHUNKS
    chunk = vp // 4 // CHUNKS
    plane, chips = 2 * vocab_count, seq_count // 2
    share = total // vocab_count
    code = Code(GAIN_MAX * UNEMBED_MAX * model * (STATE_MAX + BIAS_MAX + model * STATE_MAX * MATRIX_MAX))
    xcode = Code(STATE_MAX + BIAS_MAX + model * STATE_MAX * MATRIX_MAX)
    deep = -(-3 * layers // 8) * 8
    dma = pltpu.SemaphoreType.DMA
    vmem = pl.BlockSpec(memory_space=pltpu.VMEM)
    hbm = pl.BlockSpec(memory_space=pl.ANY)
    body = lambda *refs: kernel(layers, total, cap, seq_count, vocab_count, model, code, xcode, *refs)
    return pl.pallas_call(
        body,
        out_shape=jax.ShapeDtypeStruct((cap, 128), f32),
        in_specs=[vmem, pl.BlockSpec(memory_space=pltpu.SMEM), vmem, vmem, vmem, hbm, hbm],
        out_specs=vmem,
        scratch_shapes=[
            pltpu.VMEM((2, 2, CHUNKS, chunk, wo), bf16),
            pltpu.VMEM((layers - 1, wi, wo), bf16),
            pltpu.VMEM((1, 128), i32),
            pltpu.VMEM((layers, seq_count * cap, wi), bf16),
            pltpu.VMEM((total, wi), bf16),
            pltpu.VMEM((total, seq_count * cap), bf16),
            pltpu.VMEM((1, total), i32),
            pltpu.VMEM((cap, total), f32),
            pltpu.VMEM((seq_count, 1, 128), i32),
            pltpu.VMEM((total, wo), f32),
            pltpu.VMEM((layers, share, wo), f32),
            pltpu.VMEM((layers, total, wo), i16),
            pltpu.VMEM((layers, vocab_count, share, wo), i16),
            pltpu.VMEM((layers, total, wo), bf16),
            pltpu.VMEM((layers, vocab_count, 1, total), f32),
            pltpu.VMEM((layers, 1, total), f32),
            pltpu.VMEM((layers, seq_count, 1, total), f32),
            pltpu.VMEM((layers, 1, total), f32),
            pltpu.VMEM((steps, 2, chunk, total), f32),
            pltpu.VMEM((SLOTS, 2, chunk, total), f32),
            pltpu.VMEM((steps, 2, chunk, total), f32),
            pltpu.VMEM((2, steps, chunk, total), i16),
            pltpu.VMEM((steps, 2, chunk, total), i16),
            pltpu.VMEM((CHUNKS, chunk, total), f32),
            pltpu.VMEM((CHUNKS, chunk, total), f32),
            pltpu.VMEM((3 * layers, 8, total), f32),
            pltpu.VMEM((deep, total), f32),
            pltpu.VMEM((plane, deep, total), f32),
            pltpu.VMEM((deep, total), f32),
            pltpu.VMEM((2, deep, total), f32),
            dma((CHUNKS,)),
            dma((layers - 1,)),
            dma((1,)),
            dma((1,)),
            dma((layers, 2)),
            dma((layers, chips)),
            dma((layers,)),
            dma((layers,)),
            dma((layers,)),
            dma((layers,)),
            dma((layers,)),
            dma((layers,)),
            dma((layers,)),
            dma((layers,)),
            dma((layers,)),
            dma((layers,)),
            dma((SLOTS,)),
            dma((steps,)),
            dma((2,)),
            dma((steps, 2)),
            dma((1,)),
            dma((1,)),
            dma((1,)),
            dma((2,)),
        ],
        compiler_params=pltpu.CompilerParams(
            collective_id=0, has_side_effects=True, vmem_limit_bytes=63 << 20
        ),
        name="readout",
    )(rows, count, wanted, bias, gain, translator, unembed.reshape(2, 2, CHUNKS, chunk, wo))

def body(
    probe_states,
    final_states,
    translator,
    translator_bias,
    norm_gain,
    unembed,
    answer_rows,
    answer_count,
    targets,
):
    seq_count = lax.axis_size("seq")
    vocab_count = lax.axis_size("vocab")
    model = probe_states.shape[2] * vocab_count
    layers = probe_states.shape[0]
    out = readout(
        pick(answer_rows, probe_states, final_states),
        answer_count,
        targets,
        translator_bias,
        norm_gain,
        translator,
        unembed,
        seq_count,
        vocab_count,
        seq_count * FLAG_DEV,
        model,
    )
    flat = out[:, : 2 * layers + 1].T
    return flat[: layers + 1, None, :], flat[layers + 1 :, None, :]

def solution(mesh):
    in_specs = (
        P(None, "seq", "vocab"),
        P("seq", "vocab"),
        P(None, "vocab", "seq"),
        P(None, "seq"),
        P("seq"),
        P("vocab", "seq"),
        P("seq", None),
        P("seq"),
        P("seq", None),
    )
    out_specs = (P(None, "seq", None), P(None, "seq", None))
    return jax.shard_map(body, mesh=mesh, in_specs=in_specs, out_specs=out_specs, check_vma=False)
```
